32 devices in a mesh: batch: 2 (over x), col: 4 (over z), row: 4 (over y, core).
Axes of the slice: x: 2, y: 2, z: 4, core: 2. Of those that a mesh axis runs over, the one named last changes fastest.
Arguments:
- pair_rep: bfloat16 [1536, 768, 128], P(('batch', 'row'), 'col'), parts along dimension 0
- pair_mask: int32 [1536, 768], P(('batch', 'row'), 'col'), parts along dimension 0
- ln_in_scale: bfloat16 [128], replicated
- w_left: bfloat16 [128, 128], replicated
- w_left_gate: bfloat16 [128, 128], replicated
- w_right: bfloat16 [128, 128], replicated
- w_right_gate: bfloat16 [128, 128], replicated
- w_out_gate: bfloat16 [128, 128], replicated
- ln_out_scale: bfloat16 [128], replicated
- w_out: bfloat16 [128, 128], replicated
Outputs:
- output: bfloat16 [1536, 768, 128], P(('batch', 'row'), 'col'), parts along dimension 0
There are 2 independent parts. The reference program is written for one: setup_inputs(seed, part) draws one part's arguments, and reference() takes and returns one part's arrays. A program takes and returns all parts, laid end to end along the dimension named above; an argument that names none is the same for every part.
All inputs are finite; a program needn't handle non-finite values.
Results may differ from the reference program's by a relative error of at most 0.00119143.
Values are sent between devices in bfloat16 or wider.
A program may use at most 1 GiB of HBM per device.

```python
import math
import jax
import jax.numpy as jnp
from jax import lax

RESIDUES = 768
PAIR_DIM = 128
TRI_DIM = 128
ROW_BLK = math.gcd(RESIDUES, 64)
NUM_BLK = RESIDUES // ROW_BLK
LN_EPS = 0.00001


def layer_norm(values, gain_vec):
    mean_val = jnp.mean(values, axis=-1, keepdims=True)
    centered = values - mean_val
    variance = jnp.mean(centered * centered, axis=-1, keepdims=True)
    return centered * lax.rsqrt(variance + LN_EPS) * gain_vec.astype(jnp.float32)


def setup_inputs(seed: int = 0, part: int = 0) -> dict:
    part_keys = jax.random.split(jax.random.fold_in(jax.random.key(seed), part), 3)
    weight_keys = jax.random.split(jax.random.key(seed + 1), 8)
    pair_rep = jax.random.normal(part_keys[0], (RESIDUES, RESIDUES, PAIR_DIM), jnp.float32).astype(jnp.bfloat16)
    residue_ok = jax.random.randint(part_keys[1], (RESIDUES,), 0, 16) != 0
    pair_ok = jax.random.randint(part_keys[2], (RESIDUES, RESIDUES), 0, 8) != 0
    pair_mask = (residue_ok[:, None] & residue_ok[None, :] & pair_ok).astype(jnp.int32)

    def matrix(key_val, fan_in, fan_out):
        return (jax.random.normal(key_val, (fan_in, fan_out), jnp.float32) * fan_in ** -0.5).astype(jnp.bfloat16)

    def gain_vector(key_val, num_chan):
        return (1.0 + 0.5 * jax.random.normal(key_val, (num_chan,), jnp.float32)).astype(jnp.bfloat16)

    return {
        'pair_rep': pair_rep,
        'pair_mask': pair_mask,
        'ln_in_scale': gain_vector(weight_keys[0], PAIR_DIM),
        'w_left': matrix(weight_keys[1], PAIR_DIM, TRI_DIM),
        'w_left_gate': matrix(weight_keys[2], PAIR_DIM, TRI_DIM),
        'w_right': matrix(weight_keys[3], PAIR_DIM, TRI_DIM),
        'w_right_gate': matrix(weight_keys[4], PAIR_DIM, TRI_DIM),
        'w_out_gate': matrix(weight_keys[5], PAIR_DIM, PAIR_DIM),
        'ln_out_scale': gain_vector(weight_keys[6], TRI_DIM),
        'w_out': matrix(weight_keys[7], TRI_DIM, PAIR_DIM),
    }


def reference(pair_rep, pair_mask, ln_in_scale, w_left, w_left_gate, w_right, w_right_gate, w_out_gate, ln_out_scale, w_out):
    pair_blocks = pair_rep.reshape(NUM_BLK, ROW_BLK, RESIDUES, PAIR_DIM)
    mask_blocks = pair_mask.reshape(NUM_BLK, ROW_BLK * RESIDUES, 1).astype(jnp.float32)

    def project(block_args):
        pair_rows, keep_rows = block_args
        normed = layer_norm(pair_rows.astype(jnp.float32), ln_in_scale).astype(jnp.bfloat16).reshape(ROW_BLK * RESIDUES, PAIR_DIM)
        left_act = keep_rows * jax.nn.sigmoid(jnp.dot(normed, w_left_gate, preferred_element_type=jnp.float32)) * jnp.dot(normed, w_left, preferred_element_type=jnp.float32)
        right_act = keep_rows * jax.nn.sigmoid(jnp.dot(normed, w_right_gate, preferred_element_type=jnp.float32)) * jnp.dot(normed, w_right, preferred_element_type=jnp.float32)
        return left_act.astype(jnp.bfloat16), right_act.astype(jnp.bfloat16)

    left_all, right_all = lax.map(project, (pair_blocks, mask_blocks))
    right_t = right_all.reshape(RESIDUES, RESIDUES, TRI_DIM).astype(jnp.float32).transpose(2, 0, 1)
    left_blocks = left_all.reshape(RESIDUES, NUM_BLK, ROW_BLK, TRI_DIM).transpose(1, 3, 0, 2)

    def finish(block_args):
        left_cols, pair_rows = block_args
        summed = jnp.einsum('hki,hkj->ijh', left_cols.astype(jnp.float32), right_t)
        normed_out = layer_norm(summed, ln_out_scale).astype(jnp.bfloat16).reshape(ROW_BLK * RESIDUES, TRI_DIM)
        update = jnp.dot(normed_out, w_out, preferred_element_type=jnp.float32)
        pair_flat = pair_rows.astype(jnp.float32).reshape(ROW_BLK * RESIDUES, PAIR_DIM)
        normed_in = layer_norm(pair_flat, ln_in_scale).astype(jnp.bfloat16)
        gate_act = jax.nn.sigmoid(jnp.dot(normed_in, w_out_gate, preferred_element_type=jnp.float32))
        return (pair_flat + gate_act * update).astype(jnp.bfloat16).reshape(ROW_BLK, RESIDUES, PAIR_DIM)

    return lax.map(finish, (left_blocks, pair_blocks)).reshape(RESIDUES, RESIDUES, PAIR_DIM)
```

```python
import jax
import jax.numpy as jnp
from jax import lax
from jax.experimental import pallas as pl
from jax.experimental.pallas import tpu as pltpu
from jax.sharding import PartitionSpec as P

LN_EPS = 0.00001
AXES = ('col', 'row')
BF16, F32 = jnp.bfloat16, jnp.float32
VMEM_BYTES = 60 * 2**20
FLOPS_PER_US = 250_000_000


def moves(target):
    pairs = []
    for z in range(4):
        for y in range(2):
            for c in range(2):
                to = target(y, z, c)
                if to is not None:
                    pairs.append((z * 4 + y * 2 + c, to[1] * 4 + to[0] * 2 + to[2]))
    return pairs


TO_Y = moves(lambda y, z, c: (1 - y, z, c))
TO_Z = moves(lambda y, z, c: (y, z ^ 1, c))
TO_CORE = moves(lambda y, z, c: (y, z, 1 - c))
ACROSS = moves(lambda y, z, c: (y, 3 - z if z in (1, 2) else z, c))


def home(from_y, turn):
    def target(y, z, c):
        if y != from_y:
            return None
        half = z // 2
        block_half = 1 - half if z in (1, 2) else half
        return (block_half, 2 * half + c, half ^ turn)
    return moves(target)


def send(value, pairs):
    return lax.ppermute(value, AXES, pairs)


def after(value, *others):
    return lax.optimization_barrier((value,) + others)[0]


def cost(us, nbytes):
    return pl.CostEstimate(flops=us * FLOPS_PER_US, bytes_accessed=nbytes, transcendentals=0)


def params():
    return pltpu.CompilerParams(vmem_limit_bytes=VMEM_BYTES)


def normed(values, gain):
    mean_val = jnp.mean(values, axis=-1, keepdims=True)
    centered = values - mean_val
    variance = jnp.mean(centered * centered, axis=-1, keepdims=True)
    return (centered * lax.rsqrt(variance + LN_EPS) * gain).astype(BF16)


def dot_nt(lhs, rhs):
    return lax.dot_general(lhs, rhs, (((1,), (1,)), ((), ())), preferred_element_type=F32)


def project_body(pieces, gain_ref, w_ref, out_refs, s_ref):
    tri = s_ref.shape[1]
    gain = gain_ref[...].astype(F32)
    x = jnp.concatenate([normed(p.astype(F32), gain) for p in pieces], axis=0)
    x = jnp.swapaxes(x, 0, 1)
    for i in range(x.shape[0]):
        proj = dot_nt(w_ref[...], x[i])
        s_ref[i] = jax.nn.sigmoid(proj[tri:]) * proj[:tri]
    part = tri // len(out_refs)
    for q, out_ref in enumerate(out_refs):
        out_ref[...] = jnp.swapaxes(s_ref[:, q * part:(q + 1) * part, :], 0, 1).astype(BF16)


def project_kernel(p0_ref, p1_ref, gain_ref, w_ref, *refs):
    project_body((p0_ref[...], p1_ref[...]), gain_ref, w_ref, refs[:-1], refs[-1])


def project_pick_kernel(flag_ref, p0_ref, p1_ref, q0_ref, q1_ref, gain_ref, w_ref, out_ref, s_ref):
    pick = flag_ref[0] != 0
    project_body((jnp.where(pick, p0_ref[...], q0_ref[...]), jnp.where(pick, p1_ref[...], q1_ref[...])), gain_ref, w_ref, (out_ref,), s_ref)


def project(pieces, gain, w_t, n_out=1, blk=16):
    rows, cols, dim = pieces[0].shape
    wide = w_t.shape[0]
    tri = wide // 2
    return pl.pallas_call(
        project_kernel,
        grid=(cols // blk,),
        in_specs=[pl.BlockSpec((rows, blk, dim), lambda g: (0, g, 0))] * 2
        + [pl.BlockSpec((1, dim), lambda g: (0, 0)), pl.BlockSpec((wide, dim), lambda g: (0, 0))],
        out_specs=[pl.BlockSpec((tri // n_out, blk, 2 * rows), lambda g: (0, g, 0))] * n_out,
        out_shape=[jax.ShapeDtypeStruct((tri // n_out, cols, 2 * rows), BF16)] * n_out,
        scratch_shapes=[pltpu.VMEM((blk, tri, 2 * rows), F32)],
        compiler_params=params(),
        cost_estimate=cost(23, 4 * rows * cols * (dim + tri)),
        name='project',
    )(*pieces, gain, w_t)


def project_pick(flag, yes, no, gain, w_t, blk=16):
    rows, cols, dim = yes[0].shape
    wide = w_t.shape[0]
    tri = wide // 2
    return pl.pallas_call(
        project_pick_kernel,
        grid_spec=pltpu.PrefetchScalarGridSpec(
            num_scalar_prefetch=1,
            grid=(cols // blk,),
            in_specs=[pl.BlockSpec((rows, blk, dim), lambda g, f: (0, g * f[0], 0))] * 2
            + [pl.BlockSpec((rows, blk, dim), lambda g, f: (0, g * (1 - f[0]), 0))] * 2
            + [pl.BlockSpec((1, dim), lambda g, f: (0, 0)), pl.BlockSpec((wide, dim), lambda g, f: (0, 0))],
            out_specs=pl.BlockSpec((tri, blk, 2 * rows), lambda g, f: (0, g, 0)),
            scratch_shapes=[pltpu.VMEM((blk, tri, 2 * rows), F32)],
        ),
        out_shape=jax.ShapeDtypeStruct((tri, cols, 2 * rows), BF16),
        compiler_params=params(),
        cost_estimate=cost(23, 4 * rows * cols * (dim + tri)),
        name='project_pick',
    )(flag, *yes, *no, gain, w_t)


def triangle_kernel(n_chunk, *refs):
    a_refs, refs = refs[:2 * n_chunk], refs[2 * n_chunk:]
    b_refs, (gain_ref, out_ref, *o_refs) = refs[:4], refs[4:]
    step, steps = pl.program_id(0), pl.num_programs(0)
    n_h, n_i, _ = a_refs[0].shape
    tri = n_h * steps
    pitch = o_refs[0].shape[0] // tri
    n_j = out_ref.shape[1]

    def accumulate(a0_ref, a1_ref):
        for h in range(n_h):
            acc = dot_nt(a0_ref[h], jnp.concatenate([b_refs[0][h], b_refs[1][h]], axis=0))
            acc += dot_nt(a1_ref[h], jnp.concatenate([b_refs[2][h], b_refs[3][h]], axis=0))
            start = pl.multiple_of((step * n_h + h) * pitch, 8)
            for at, o_ref in zip(range(0, n_j, 128), o_refs):
                width = min(128, n_j - at)
                o_ref[pl.ds(start, n_i), :width] = acc[:, at:at + width]

    for q in range(n_chunk):
        @pl.when(step // (steps // n_chunk) == q)
        def _(q=q):
            accumulate(a_refs[2 * q], a_refs[2 * q + 1])

    @pl.when(step == steps - 1)
    def _():
        gain = gain_ref[...].astype(F32)

        @pl.loop(0, n_i)
        def _(i):
            for at, o_ref in zip(range(0, n_j, 128), o_refs):
                width = min(128, n_j - at)
                values = o_ref[pl.ds(i, tri, stride=pitch), :][:, :width]
                mean_val = jnp.mean(values, axis=0, keepdims=True)
                centered = values - mean_val
                variance = jnp.mean(centered * centered, axis=0, keepdims=True)
                unit = centered * lax.rsqrt(variance + LN_EPS)
                out_ref[i, pl.ds(at, width), :] = (unit.T * gain).astype(BF16)


def triangle(a_chunks, b_parts, gain, blk=8):
    n_chunk = len(a_chunks)
    part, n_i, n_k = a_chunks[0][0].shape
    tri, half_j, _ = b_parts[0].shape
    n_j = 2 * half_j
    per = part // blk
    a_specs = []
    for q in range(n_chunk):
        a_specs += [pl.BlockSpec((blk, n_i, n_k), lambda g, q=q: (jnp.clip(g - q * per, 0, per - 1), 0, 0))] * 2
    pitch = n_i + 8
    return pl.pallas_call(
        lambda *refs: triangle_kernel(n_chunk, *refs),
        grid=(tri // blk,),
        in_specs=a_specs + [pl.BlockSpec((blk, half_j, n_k), lambda g: (g, 0, 0))] * 4 + [pl.BlockSpec((1, tri), lambda g: (0, 0))],
        out_specs=pl.BlockSpec((n_i, n_j, tri), lambda g: (0, 0, 0)),
        out_shape=jax.ShapeDtypeStruct((n_i, n_j, tri), BF16),
        scratch_shapes=[pltpu.VMEM((tri * pitch, 128), F32)] * pl.cdiv(n_j, 128),
        compiler_params=params(),
        cost_estimate=cost(45, 2 * tri * n_k * 2 * (n_i + n_j)),
        name='triangle',
    )(*[a for pair in a_chunks for a in pair], *b_parts, gain)


def finish_kernel(flag_ref, z_ref, y00_ref, y01_ref, y10_ref, y11_ref, gain_ref, wg_ref, wo_ref, out_ref):
    rows, cols, dim = z_ref.shape
    first = flag_ref[0] == 0
    y0 = jnp.where(first, y00_ref[...], y01_ref[...])
    y1 = jnp.where(first, y10_ref[...], y11_ref[...])
    normed_out = jnp.where(pl.program_id(0) == 0, y0, y1).reshape(rows * cols, -1)
    pair = z_ref[...].astype(F32).reshape(rows * cols, dim)
    x = normed(pair, gain_ref[...].astype(F32))
    gate = jax.nn.sigmoid(jnp.dot(x, wg_ref[...], preferred_element_type=F32))
    update = jnp.dot(normed_out, wo_ref[...], preferred_element_type=F32)
    out_ref[...] = (pair + gate * update).astype(BF16).reshape(rows, cols, dim)


def finish(flag, pair_tile, got, gain, w_gate, w_out, blk=24):
    rows, cols, dim = pair_tile.shape
    half_rows, half_cols = rows // 2, cols // 2
    blk = min(blk, half_rows)
    per = half_rows // blk
    tri = got[0][0].shape[2]

    def y_spec(from_y, turn):
        def index(s, g, j, f):
            on = (s == from_y) & (f[0] == turn)
            return jnp.where(on, g, 0), jnp.where(on, j ^ from_y, 0), 0
        return pl.BlockSpec((blk, half_cols, tri), index)

    z_spec = pl.BlockSpec((blk, half_cols, dim), lambda s, g, j, f: (s * per + g, j, 0))
    whole = [pl.BlockSpec(v.shape, lambda s, g, j, f: (0, 0)) for v in (gain, w_gate, w_out)]
    return pl.pallas_call(
        finish_kernel,
        grid_spec=pltpu.PrefetchScalarGridSpec(
            num_scalar_prefetch=1,
            grid=(2, per, 2),
            in_specs=[z_spec] + [y_spec(s, t) for s in (0, 1) for t in (0, 1)] + whole,
            out_specs=z_spec,
        ),
        out_shape=jax.ShapeDtypeStruct(pair_tile.shape, BF16),
        compiler_params=params(),
        cost_estimate=cost(21, 6 * rows * cols * dim),
        name='finish',
    )(flag, pair_tile, got[0][0], got[0][1], got[1][0], got[1][1], gain, w_gate, w_out)


def solution(mesh):
    tile_spec = P(('batch', 'row'), 'col', None)
    mask_spec = P(('batch', 'row'), 'col')
    replicated = P()

    def local_step(pair_tile, mask_tile, ln_in_scale, w_left, w_left_gate, w_right, w_right_gate, w_out_gate, ln_out_scale, w_out):
        rows, cols, dim = pair_tile.shape
        half_cols = cols // 2
        tri = w_left.shape[1]
        row, z = lax.axis_index('row'), lax.axis_index('col')
        y, c = row // 2, row % 2
        half = z // 2
        w_a = jnp.concatenate([w_left, w_left_gate], axis=1).T
        w_b = jnp.concatenate([w_right, w_right_gate], axis=1).T
        gain_in, gain_out = ln_in_scale[None], ln_out_scale[None]

        masked = jnp.where((mask_tile != 0)[:, :, None], pair_tile, jnp.zeros((), BF16))
        t_a = lax.dynamic_slice_in_dim(masked, y * half_cols, half_cols, 1)
        t_b = lax.dynamic_slice_in_dim(masked, (1 - y) * half_cols, half_cols, 1)
        y_a = send(t_b, TO_Y)
        z_a = send(t_a, TO_Z)
        m_0 = send(t_a, ACROSS)
        y_b = send(after(t_a, z_a), TO_Y)
        yz_a = send(y_a, TO_Z)
        m_1 = send(after(y_a, m_0), ACROSS)
        z_b = send(after(t_b, yz_a), TO_Z)
        yz_b = send(after(z_a, y_b), TO_Y)

        a_1_own, last = [], m_1
        for part in project((z_a, yz_a), gain_in, w_a, n_out=2):
            last = send(after(part, last), ACROSS)
            a_1_own.append(last)
        a_0_own, = project((m_0, m_1), gain_in, w_a)
        a_turns = [[(a_0_own, send(a_0_own, TO_CORE))], [(v, send(v, TO_CORE)) for v in a_1_own]]

        own_col = (z % 2) == c
        keep = own_col.astype(jnp.int32)[None]
        sets = [((t_a, y_a), (z_a, yz_a)), ((t_b, y_b), (z_b, yz_b))]
        b_give = [project_pick(1 - keep, own, other, gain_in, w_b) for own, other in sets]
        b_sib = [send(v, TO_CORE) for v in b_give]
        b_keep = [project_pick(keep, own, other, gain_in, w_b) for own, other in sets]

        halves = [triangle(a_turns[0], b_keep + b_sib, gain_out)]
        halves.append(triangle(a_turns[1], b_keep + b_sib, after(gain_out, halves[0])))
        got = [[send(halves[turn], home(from_y, turn)) for turn in (0, 1)] for from_y in (0, 1)]
        flag = (half ^ c).astype(jnp.int32)[None]
        return finish(flag, pair_tile, got, gain_in, w_out_gate, w_out)

    return jax.shard_map(local_step, mesh=mesh, in_specs=(tile_spec, mask_spec) + (replicated,) * 8, out_specs=tile_spec, check_vma=False)
```

```python
import jax
import jax.numpy as jnp
from jax import lax
from jax.experimental import pallas as pl
from jax.experimental.pallas import tpu as pltpu
from jax.sharding import PartitionSpec as P


LN_EPS = 0.00001
AXES = ('col', 'row')
BF16, F32 = jnp.bfloat16, jnp.float32
VMEM_BYTES = 60 * 2**20
FLOPS_PER_US = 5_000_000


def moves(target):
    pairs = []
    for z in range(4):
        for y in range(2):
            for c in range(2):
                to = target(y, z, c)
                if to is not None:
                    pairs.append((z * 4 + y * 2 + c, to[1] * 4 + to[0] * 2 + to[2]))
    return pairs


TO_Y = moves(lambda y, z, c: (1 - y, z, c))
TO_Z = moves(lambda y, z, c: (y, z ^ 1, c))
TO_CORE = moves(lambda y, z, c: (y, z, 1 - c))
ACROSS = moves(lambda y, z, c: (y, 3 - z if z in (1, 2) else z, c))


def home(from_y, turn):
    def target(y, z, c):
        if y != from_y:
            return None
        half = z // 2
        block_half = 1 - half if z in (1, 2) else half
        to = (block_half, 2 * half + c, half ^ turn)
        return None if to == (y, z, c) else to

    return moves(target)


def send(value, pairs):
    return lax.ppermute(value, AXES, pairs)


def after(value, *others):
    return lax.optimization_barrier((value,) + others)[0]


def cost(us, nbytes):
    return pl.CostEstimate(flops=us * FLOPS_PER_US, bytes_accessed=nbytes, transcendentals=0)


def params():
    return pltpu.CompilerParams(vmem_limit_bytes=VMEM_BYTES)


def normed(values, gain):
    mean_val = jnp.mean(values, axis=-1, keepdims=True)
    centered = values - mean_val
    variance = jnp.mean(centered * centered, axis=-1, keepdims=True)
    return (centered * lax.rsqrt(variance + LN_EPS) * gain).astype(BF16)


def dot_nt(lhs, rhs):
    return lax.dot_general(lhs, rhs, (((1,), (1,)), ((), ())), preferred_element_type=F32)


def project_body(pieces, gain_ref, w_ref, out_refs, s_ref):
    tri = s_ref.shape[1]
    gain = gain_ref[...].astype(F32)
    x = jnp.concatenate([normed(p.astype(F32), gain) for p in pieces], axis=0)
    x = jnp.swapaxes(x, 0, 1)
    for i in range(x.shape[0]):
        proj = dot_nt(w_ref[...], x[i])
        s_ref[i] = jax.nn.sigmoid(proj[tri:]) * proj[:tri]
    part = tri // len(out_refs)
    for q, out_ref in enumerate(out_refs):
        out_ref[...] = jnp.swapaxes(s_ref[:, q * part:(q + 1) * part, :], 0, 1).astype(BF16)


def project_kernel(p0_ref, p1_ref, gain_ref, w_ref, *refs):
    project_body((p0_ref[...], p1_ref[...]), gain_ref, w_ref, refs[:-1], refs[-1])


def project_pick_kernel(flag_ref, p0_ref, p1_ref, q0_ref, q1_ref, gain_ref, w_ref, out_ref, s_ref):
    pick = flag_ref[0] != 0
    project_body((jnp.where(pick, p0_ref[...], q0_ref[...]), jnp.where(pick, p1_ref[...], q1_ref[...])), gain_ref, w_ref, (out_ref,), s_ref)


def project(pieces, gain, w_t, n_out=1, blk=16):
    rows, cols, dim = pieces[0].shape
    wide = w_t.shape[0]
    tri = wide // 2
    return pl.pallas_call(
        project_kernel,
        grid=(cols // blk,),
        in_specs=[pl.BlockSpec((rows, blk, dim), lambda g: (0, g, 0))] * 2
        + [pl.BlockSpec((1, dim), lambda g: (0, 0)), pl.BlockSpec((wide, dim), lambda g: (0, 0))],
        out_specs=[pl.BlockSpec((tri // n_out, blk, 2 * rows), lambda g: (0, g, 0))] * n_out,
        out_shape=[jax.ShapeDtypeStruct((tri // n_out, cols, 2 * rows), BF16)] * n_out,
        scratch_shapes=[pltpu.VMEM((blk, tri, 2 * rows), F32)],
        compiler_params=params(),
        cost_estimate=cost(23, 4 * rows * cols * (dim + tri)),
        name='project',
    )(*pieces, gain, w_t)


def project_pick(flag, yes, no, gain, w_t, blk=16):
    rows, cols, dim = yes[0].shape
    wide = w_t.shape[0]
    tri = wide // 2
    return pl.pallas_call(
        project_pick_kernel,
        grid_spec=pltpu.PrefetchScalarGridSpec(
            num_scalar_prefetch=1,
            grid=(cols // blk,),
            in_specs=[pl.BlockSpec((rows, blk, dim), lambda g, f: (0, g * f[0], 0))] * 2
            + [pl.BlockSpec((rows, blk, dim), lambda g, f: (0, g * (1 - f[0]), 0))] * 2
            + [pl.BlockSpec((1, dim), lambda g, f: (0, 0)), pl.BlockSpec((wide, dim), lambda g, f: (0, 0))],
            out_specs=pl.BlockSpec((tri, blk, 2 * rows), lambda g, f: (0, g, 0)),
            scratch_shapes=[pltpu.VMEM((blk, tri, 2 * rows), F32)],
        ),
        out_shape=jax.ShapeDtypeStruct((tri, cols, 2 * rows), BF16),
        compiler_params=params(),
        cost_estimate=cost(23, 4 * rows * cols * (dim + tri)),
        name='project_pick',
    )(flag, *yes, *no, gain, w_t)


def triangle_kernel(n_prev, last, *refs):
    (a0_ref, a1_ref), b_refs, refs = refs[:2], refs[2:6], refs[6:]
    step, steps = pl.program_id(0), pl.num_programs(0)
    n_h, n_i, _ = a0_ref.shape
    n_j = 2 * b_refs[0].shape[1]
    pitch = n_i + 8
    spans = [(at, min(128, n_j - at)) for at in range(0, n_j, 128)]
    n_o = len(spans)
    if last:
        prev_refs, gain_ref, out_ref, o_refs = refs[:n_o * n_prev], refs[n_o * n_prev], refs[n_o * n_prev + 1], refs[n_o * n_prev + 2:]
    else:
        o_refs = refs
    base = (step + n_prev * steps) * n_h if last else 0
    for h in range(n_h):
        acc = dot_nt(a0_ref[h], jnp.concatenate([b_refs[0][h], b_refs[1][h]], axis=0))
        acc += dot_nt(a1_ref[h], jnp.concatenate([b_refs[2][h], b_refs[3][h]], axis=0))
        start = pl.multiple_of((base + h) * pitch, 8)
        for (at, width), o_ref in zip(spans, o_refs):
            o_ref[pl.ds(start, n_i), :width] = acc[:, at:at + width]
    if not last:
        return
    if n_prev:
        for prev_ref, o_ref in zip(prev_refs, o_refs):
            o_ref[pl.ds(pl.multiple_of(step * n_h * pitch, 8), n_h * pitch), :] = prev_ref[...]

    @pl.when(step == steps - 1)
    def _():
        tri = o_refs[0].shape[0] // pitch
        gain = gain_ref[...].astype(F32)

        @pl.loop(0, n_i)
        def _(i):
            for (at, width), o_ref in zip(spans, o_refs):
                values = o_ref[pl.ds(i, tri, stride=pitch), :][:, :width]
                mean_val = jnp.mean(values, axis=0, keepdims=True)
                centered = values - mean_val
                variance = jnp.mean(centered * centered, axis=0, keepdims=True)
                unit = centered * lax.rsqrt(variance + LN_EPS)
                out_ref[i, pl.ds(at, width), :] = (unit.T * gain).astype(BF16)


def triangle(a_pair, b_parts, gain, first=0, prev=None, last=True, blk=8):
    part, n_i, n_k = a_pair[0].shape
    tri, half_j, _ = b_parts[0].shape
    n_j = 2 * half_j
    pitch, n_o = n_i + 8, pl.cdiv(n_j, 128)
    n_prev = 0 if prev is None else 1
    o_spec = pl.BlockSpec((blk * pitch, 128), lambda g: (g, 0))
    in_specs = [pl.BlockSpec((blk, n_i, n_k), lambda g: (g, 0, 0))] * 2
    in_specs += [pl.BlockSpec((blk, half_j, n_k), lambda g: (g + first // blk, 0, 0))] * 4
    operands = [*a_pair, *b_parts]
    if last:
        in_specs += [o_spec] * (n_o * n_prev) + [pl.BlockSpec((1, tri), lambda g: (0, 0))]
        operands += list(prev or []) + [gain]
        out_specs = pl.BlockSpec((n_i, n_j, tri), lambda g: (0, 0, 0))
        out_shape = jax.ShapeDtypeStruct((n_i, n_j, tri), BF16)
        scratch = [pltpu.VMEM((tri * pitch, 128), F32)] * n_o
    else:
        out_specs = [o_spec] * n_o
        out_shape = [jax.ShapeDtypeStruct((part * pitch, 128), F32)] * n_o
        scratch = []
    return pl.pallas_call(
        lambda *refs: triangle_kernel(n_prev, last, *refs),
        grid=(part // blk,),
        in_specs=in_specs,
        out_specs=out_specs,
        out_shape=out_shape,
        scratch_shapes=scratch,
        compiler_params=params(),
        cost_estimate=cost(30 * part // tri + (15 if last else 0), 2 * part * n_k * 2 * (n_i + n_j)),
        name='triangle',
    )(*operands)


def gate_kernel(z_ref, gain_ref, wg_ref, out_ref):
    rows, cols, dim = z_ref.shape
    x = normed(z_ref[...].astype(F32).reshape(rows * cols, dim), gain_ref[...].astype(F32))
    out_ref[...] = jax.nn.sigmoid(jnp.dot(x, wg_ref[...], preferred_element_type=F32)).reshape(rows, cols, dim)


def out_gate(pair_tile, gain, w_gate, blk=16):
    rows, cols, dim = pair_tile.shape
    blk = min(blk, rows)
    spec = pl.BlockSpec((blk, cols, dim), lambda g: (g, 0, 0))
    return pl.pallas_call(
        gate_kernel,
        grid=(rows // blk,),
        in_specs=[spec, pl.BlockSpec((1, dim), lambda g: (0, 0)), pl.BlockSpec((dim, dim), lambda g: (0, 0))],
        out_specs=spec,
        out_shape=jax.ShapeDtypeStruct(pair_tile.shape, F32),
        compiler_params=params(),
        cost_estimate=cost(18, 6 * rows * cols * dim),
        name='out_gate',
    )(pair_tile, gain, w_gate)


def finish_kernel(pick_ref, z_ref, gate_ref, *refs):
    y_refs, wo_ref, out_ref = refs[:-2], refs[-2], refs[-1]
    rows, cols, dim = z_ref.shape
    n_cand = len(y_refs) // 2

    for s in (0, 1):
        for q in range(n_cand):
            @pl.when((pl.program_id(0) == s) & (pick_ref[s] == q))
            def _(y_ref=y_refs[s * n_cand + q]):
                update = jnp.dot(y_ref[...].reshape(rows * cols, -1), wo_ref[...], preferred_element_type=F32)
                out_ref[...] = (z_ref[...].astype(F32) + gate_ref[...] * update.reshape(rows, cols, dim)).astype(BF16)


def finish(pick, pair_tile, gate, candidates, w_out, blk=24):
    rows, cols, dim = pair_tile.shape
    half_rows, half_cols = rows // 2, cols // 2
    blk = min(blk, half_rows)
    per = half_rows // blk
    tri = w_out.shape[0]

    def y_spec(half, cand):
        def index(s, g, j, pick_ref):
            on = (s == half) & (pick_ref[half] == cand)
            return jnp.where(on, g, 0), jnp.where(on, j ^ half, 0), 0

        return pl.BlockSpec((blk, half_cols, tri), index)

    tile_spec = pl.BlockSpec((blk, half_cols, dim), lambda s, g, j, pick_ref: (s * per + g, j, 0))
    y_specs = [y_spec(s, q) for s in (0, 1) for q in range(len(candidates[s]))]
    return pl.pallas_call(
        finish_kernel,
        grid_spec=pltpu.PrefetchScalarGridSpec(
            num_scalar_prefetch=1,
            grid=(2, per, 2),
            in_specs=[tile_spec, tile_spec] + y_specs + [pl.BlockSpec(w_out.shape, lambda s, g, j, pick_ref: (0, 0))],
            out_specs=tile_spec,
        ),
        out_shape=jax.ShapeDtypeStruct(pair_tile.shape, BF16),
        compiler_params=params(),
        cost_estimate=cost(16, 10 * rows * cols * dim),
        name='finish',
    )(pick, pair_tile, gate, *candidates[0], *candidates[1], w_out)


def solution(mesh):
    tile_spec = P(('batch', 'row'), 'col', None)
    mask_spec = P(('batch', 'row'), 'col')
    replicated = P()

    def local_step(pair_tile, mask_tile, ln_in_scale, w_left, w_left_gate, w_right, w_right_gate, w_out_gate, ln_out_scale, w_out):
        _, cols, _ = pair_tile.shape
        half_cols = cols // 2
        tri = w_left.shape[1]
        row, z = lax.axis_index('row'), lax.axis_index('col')
        y, c = row // 2, row % 2
        half = z // 2
        w_a = jnp.concatenate([w_left, w_left_gate], axis=1).T
        w_b = jnp.concatenate([w_right, w_right_gate], axis=1).T
        gain_in, gain_out = ln_in_scale[None], ln_out_scale[None]

        masked = jnp.where((mask_tile != 0)[:, :, None], pair_tile, jnp.zeros((), BF16))
        t_a = jnp.where(y == 0, masked[:, :half_cols], masked[:, half_cols:])
        t_b = jnp.where(y == 0, masked[:, half_cols:], masked[:, :half_cols])
        gate = out_gate(pair_tile, gain_in, w_out_gate)
        y_a = send(t_b, TO_Y)
        z_a = send(t_a, TO_Z)
        m_0 = send(t_a, ACROSS)
        y_b = send(after(t_a, z_a), TO_Y)
        yz_a = send(after(y_a, gate), TO_Z)
        m_1 = send(y_a, ACROSS)
        z_b = send(after(t_b, yz_a), TO_Z)
        yz_b = send(after(z_a, y_b), TO_Y)

        keep = ((z % 2) == c).astype(jnp.int32)[None]
        sets = [((t_a, y_a), (z_a, yz_a)), ((t_b, y_b), (z_b, yz_b))]
        a_1 = project((z_a, yz_a), gain_in, w_a, n_out=2)
        a_1_own = [send(part, ACROSS) for part in a_1]
        give_0 = project_pick(1 - keep, *sets[0], gain_in, after(w_b, a_1[0]))
        a_0_own, = project((m_0, m_1), gain_in, after(w_a, give_0))
        a_0_sib = send(a_0_own, TO_CORE)
        keep_0 = project_pick(keep, *sets[0], gain_in, after(w_b, a_0_own))
        give_1 = project_pick(1 - keep, *sets[1], gain_in, after(w_b, keep_0))
        keep_1 = project_pick(keep, *sets[1], gain_in, after(w_b, give_1))
        b_parts = [keep_0, keep_1, send(give_0, TO_CORE), send(give_1, TO_CORE)]

        done_0 = triangle((a_0_own, a_0_sib), b_parts, gain_out)
        a_2_sib = send(a_1_own[0], TO_CORE)
        part_1 = triangle((after(a_1_own[0], done_0), a_2_sib), b_parts, gain_out, last=False)
        a_3_sib = send(after(a_1_own[1], part_1[0]), TO_CORE)
        done_1 = triangle((a_1_own[1], a_3_sib), b_parts, gain_out, first=tri // 2, prev=part_1)
        done = (done_0, done_1)

        got = [[send(done[turn], home(from_y, turn)) for turn in (0, 1)] for from_y in (0, 1)]
        inner = (z == 1) | (z == 2)
        block_half = jnp.where(inner, 1 - half, half)
        turn = half ^ c
        own = (block_half == y) & (2 * half + c == z)
        pick = jnp.stack([turn + jnp.where(own & (y == from_y), 2, 0) for from_y in (0, 1)]).astype(jnp.int32)
        return finish(pick, pair_tile, gate, [list(got[from_y]) + list(done) for from_y in (0, 1)], w_out)

    return jax.shard_map(local_step, mesh=mesh, in_specs=(tile_spec, mask_spec) + (replicated,) * 8, out_specs=tile_spec, check_vma=False)
```

```python
import jax
import jax.numpy as jnp
from jax import lax
from jax.experimental import pallas as pl
from jax.experimental.pallas import tpu as pltpu
from jax.sharding import PartitionSpec as P


LN_EPS = 0.00001
AXES = ('col', 'row')
BF16, F32 = jnp.bfloat16, jnp.float32
VMEM_BYTES = 60 * 2**20
FLOPS_PER_US = 5_000_000


def moves(target):
    pairs = []
    for z in range(4):
        for y in range(2):
            for c in range(2):
                to = target(y, z, c)
                if to is not None:
                    pairs.append((z * 4 + y * 2 + c, to[1] * 4 + to[0] * 2 + to[2]))
    return pairs


TO_Y = moves(lambda y, z, c: (1 - y, z, c))
TO_Z = moves(lambda y, z, c: (y, z ^ 1, c))
TO_CORE = moves(lambda y, z, c: (y, z, 1 - c))
ACROSS = moves(lambda y, z, c: (y, 3 - z, c) if z in (1, 2) else None)
INNER_CORE = moves(lambda y, z, c: (y, z, 1 - c) if z in (1, 2) else None)
OUTER_CORE = moves(lambda y, z, c: (y, z, 1 - c) if z in (0, 3) else None)


def home(from_y, turn):
    def target(y, z, c):
        if y != from_y:
            return None
        half = z // 2
        block_half = 1 - half if z in (1, 2) else half
        to = (block_half, 2 * half + c, half ^ turn)
        return None if to == (y, z, c) else to

    return moves(target)


def send(value, pairs):
    return lax.ppermute(value, AXES, pairs)


def after(value, *others):
    return lax.optimization_barrier((value,) + others)[0]


def cost(us, nbytes):
    return pl.CostEstimate(flops=us * FLOPS_PER_US, bytes_accessed=nbytes, transcendentals=0)


def params():
    return pltpu.CompilerParams(vmem_limit_bytes=VMEM_BYTES)


def normed(values, gain):
    mean_val = jnp.mean(values, axis=-1, keepdims=True)
    centered = values - mean_val
    variance = jnp.mean(centered * centered, axis=-1, keepdims=True)
    return (centered * lax.rsqrt(variance + LN_EPS) * gain).astype(BF16)


def dot_nt(lhs, rhs):
    return lax.dot_general(lhs, rhs, (((1,), (1,)), ((), ())), preferred_element_type=F32)


def project_body(pieces, gain_ref, w_ref, out_ref, s_ref):
    tri = s_ref.shape[1]
    gain = gain_ref[...].astype(F32)
    x = jnp.concatenate([normed(p.astype(F32), gain) for p in pieces], axis=0)
    x = jnp.swapaxes(x, 0, 1)
    for i in range(x.shape[0]):
        proj = dot_nt(w_ref[...], x[i])
        s_ref[i] = jax.nn.sigmoid(proj[tri:]) * proj[:tri]
    out_ref[...] = jnp.swapaxes(s_ref[...], 0, 1).astype(BF16)


def project_kernel(flag_ref, *refs):
    *piece_refs, gain_ref, w_ref, out_ref, s_ref = refs
    pieces = [ref[...] for ref in piece_refs]
    if len(pieces) == 4:
        pick = flag_ref[0] != 0
        pieces = [jnp.where(pick, yes, no) for yes, no in zip(pieces[:2], pieces[2:])]
    project_body(pieces, gain_ref, w_ref, out_ref, s_ref)


def project(flag, yes, no, gain, w_t, first=0, count=None, blk=16):
    rows, cols, dim = yes[0].shape
    count = count or cols
    blk = min(blk, count)
    wide = w_t.shape[0]
    tri = wide // 2
    at = first // blk
    specs = [pl.BlockSpec((rows, blk, dim), lambda g, f: (0, at + g * f[0], 0) if no else (0, at + g, 0))] * 2
    if no:
        specs += [pl.BlockSpec((rows, blk, dim), lambda g, f: (0, at + g * (1 - f[0]), 0))] * 2
    whole = [pl.BlockSpec((1, dim), lambda g, f: (0, 0)), pl.BlockSpec((wide, dim), lambda g, f: (0, 0))]
    return pl.pallas_call(
        project_kernel,
        grid_spec=pltpu.PrefetchScalarGridSpec(
            num_scalar_prefetch=1,
            grid=(count // blk,),
            in_specs=specs + whole,
            out_specs=pl.BlockSpec((tri, blk, 2 * rows), lambda g, f: (0, g, 0)),
            scratch_shapes=[pltpu.VMEM((blk, tri, 2 * rows), F32)],
        ),
        out_shape=jax.ShapeDtypeStruct((tri, count, 2 * rows), BF16),
        compiler_params=params(),
        cost_estimate=cost(23 * count // cols, 4 * rows * count * (dim + tri)),
        name='project',
    )(flag, *yes, *(no or ()), gain, w_t)


def triangle_kernel(n_pair, flag_ref, *refs):
    a_refs, b_refs = refs[:2 * n_pair], refs[2 * n_pair:2 * n_pair + 4]
    gain_ref, out_ref, *o_refs = refs[2 * n_pair + 4:]
    step, steps = pl.program_id(0), pl.num_programs(0)
    n_h, n_i, _ = a_refs[0].shape
    n_j = out_ref.shape[1]
    tri, pitch = n_h * steps, n_i + 8
    spans = [(at, min(128, n_j - at)) for at in range(0, n_j, 128)]
    pick = flag_ref[0] != 0
    for h in range(n_h):
        a_0, a_1 = a_refs[0][h], a_refs[1][h]
        if n_pair == 2:
            a_0, a_1 = jnp.where(pick, a_0, a_refs[2][h]), jnp.where(pick, a_1, a_refs[3][h])
        acc = dot_nt(a_0, jnp.concatenate([b_refs[0][h], b_refs[1][h]], axis=0))
        acc += dot_nt(a_1, jnp.concatenate([b_refs[2][h], b_refs[3][h]], axis=0))
        start = pl.multiple_of((step * n_h + h) * pitch, 8)
        for (at, width), o_ref in zip(spans, o_refs):
            o_ref[pl.ds(start, n_i), :width] = acc[:, at:at + width]

    @pl.when(step == steps - 1)
    def _():
        gain = gain_ref[...].astype(F32)

        @pl.loop(0, n_i, step=4)
        def _(first):
            for i in range(4):
                for (at, width), o_ref in zip(spans, o_refs):
                    values = o_ref[pl.ds(first + i, tri, stride=pitch), :][:, :width]
                    mean_val = jnp.mean(values, axis=0, keepdims=True)
                    centered = values - mean_val
                    variance = jnp.mean(centered * centered, axis=0, keepdims=True)
                    unit = centered * lax.rsqrt(variance + LN_EPS)
                    out_ref[first + i, pl.ds(at, width), :] = (unit.T * gain).astype(BF16)


def triangle(flag, a_pairs, b_parts, gain, blk=8):
    n_pair = len(a_pairs)
    tri, n_i, n_k = a_pairs[0][0].shape
    half_j = b_parts[0].shape[1]
    n_j = 2 * half_j
    specs = []
    for q in range(n_pair):
        specs += [pl.BlockSpec((blk, n_i, n_k), lambda g, f, q=q: (jnp.where(f[0] == 1 - q, g, 0) if n_pair == 2 else g, 0, 0))] * 2
    return pl.pallas_call(
        lambda *refs: triangle_kernel(n_pair, *refs),
        grid_spec=pltpu.PrefetchScalarGridSpec(
            num_scalar_prefetch=1,
            grid=(tri // blk,),
            in_specs=specs + [pl.BlockSpec((blk, half_j, n_k), lambda g, f: (g, 0, 0))] * 4 + [pl.BlockSpec((1, tri), lambda g, f: (0, 0))],
            out_specs=pl.BlockSpec((n_i, n_j, tri), lambda g, f: (0, 0, 0)),
            scratch_shapes=[pltpu.VMEM((tri * (n_i + 8), 128), F32)] * pl.cdiv(n_j, 128),
        ),
        out_shape=jax.ShapeDtypeStruct((n_i, n_j, tri), BF16),
        compiler_params=params(),
        cost_estimate=cost(40, 2 * tri * n_k * 2 * (n_i + n_j)),
        name='triangle',
    )(flag, *[a for pair in a_pairs for a in pair], *b_parts, gain)


def gate_kernel(z_ref, gain_ref, wg_ref, out_ref):
    rows, cols, dim = z_ref.shape
    x = normed(z_ref[...].astype(F32).reshape(rows * cols, dim), gain_ref[...].astype(F32))
    out_ref[...] = jax.nn.sigmoid(jnp.dot(x, wg_ref[...], preferred_element_type=F32)).reshape(rows, cols, dim)


def out_gate(pair_tile, gain, w_gate, blk=16):
    rows, cols, dim = pair_tile.shape
    blk = min(blk, rows)
    spec = pl.BlockSpec((blk, cols, dim), lambda g: (g, 0, 0))
    return pl.pallas_call(
        gate_kernel,
        grid=(rows // blk,),
        in_specs=[spec, pl.BlockSpec((1, dim), lambda g: (0, 0)), pl.BlockSpec((dim, dim), lambda g: (0, 0))],
        out_specs=spec,
        out_shape=jax.ShapeDtypeStruct(pair_tile.shape, F32),
        compiler_params=params(),
        cost_estimate=cost(18, 6 * rows * cols * dim),
        name='out_gate',
    )(pair_tile, gain, w_gate)


def finish_kernel(n_cand, pick_ref, z_ref, gate_ref, *refs):
    y_refs, wo_ref, out_ref = refs[:2 * n_cand], refs[2 * n_cand], refs[-1]
    rows, cols, dim = z_ref.shape
    half_cols = cols // 2
    for s in (0, 1):
        for q in range(n_cand):
            @pl.when((pl.program_id(0) == s) & (pick_ref[s] == q))
            def _(s=s, y_ref=y_refs[s * n_cand + q]):
                for j in (0, 1):
                    to, at = pl.ds(j * half_cols, half_cols), pl.ds((j ^ s) * half_cols, half_cols)
                    update = jnp.dot(y_ref[:, at, :].reshape(rows * half_cols, -1), wo_ref[...], preferred_element_type=F32)
                    total = z_ref[:, to, :].astype(F32) + gate_ref[:, to, :] * update.reshape(rows, half_cols, dim)
                    out_ref[:, to, :] = total.astype(BF16)


def finish(pick, pair_tile, gate, candidates, w_out, part, so_far=None, blk=12):
    rows, cols, dim = pair_tile.shape
    half_rows = rows // 2
    quarter = half_rows // 2
    blk = blk if quarter % blk == 0 else quarter
    per = quarter // blk
    tri = w_out.shape[0]
    n_cand = len(candidates[0])

    def y_spec(half, cand):
        skip = part * per if candidates[half][cand].shape[0] == half_rows else 0

        def index(s, g, pick_ref):
            return jnp.where((s == half) & (pick_ref[half] == cand), skip + g, 0), 0, 0

        return pl.BlockSpec((blk, cols, tri), index)

    tile_spec = pl.BlockSpec((blk, cols, dim), lambda s, g, pick_ref: (s * 2 * per + part * per + g, 0, 0))
    y_specs = [y_spec(s, q) for s in (0, 1) for q in range(n_cand)]
    operands = [pick, pair_tile, gate, *candidates[0], *candidates[1], w_out]
    specs = [tile_spec, tile_spec] + y_specs + [pl.BlockSpec(w_out.shape, lambda s, g, pick_ref: (0, 0))]
    aliases = {}
    if so_far is not None:
        aliases = {len(operands): 0}
        operands.append(so_far)
        specs.append(pl.BlockSpec(memory_space=pl.ANY))
    return pl.pallas_call(
        lambda *refs: finish_kernel(n_cand, *refs),
        grid_spec=pltpu.PrefetchScalarGridSpec(num_scalar_prefetch=1, grid=(2, per), in_specs=specs, out_specs=tile_spec),
        out_shape=jax.ShapeDtypeStruct(pair_tile.shape, BF16),
        input_output_aliases=aliases,
        compiler_params=params(),
        cost_estimate=cost(8, 5 * rows * cols * dim),
        name='finish',
    )(*operands)


def solution(mesh):
    tile_spec = P(('batch', 'row'), 'col', None)
    mask_spec = P(('batch', 'row'), 'col')
    replicated = P()

    def local_step(pair_tile, mask_tile, ln_in_scale, w_left, w_left_gate, w_right, w_right_gate, w_out_gate, ln_out_scale, w_out):
        _, cols, _ = pair_tile.shape
        half_cols = cols // 2
        row, z = lax.axis_index('row'), lax.axis_index('col')
        y, c = row // 2, row % 2
        half = z // 2
        w_a = jnp.concatenate([w_left, w_left_gate], axis=1).T
        w_b = jnp.concatenate([w_right, w_right_gate], axis=1).T
        gain_in, gain_out = ln_in_scale[None], ln_out_scale[None]

        inner = (z == 1) | (z == 2)
        inner_flag, outer_flag = inner.astype(jnp.int32)[None], (1 - inner.astype(jnp.int32))[None]

        def masked(pairs, mask, upper):
            pairs = jnp.where(upper, pairs[:, half_cols:], pairs[:, :half_cols])
            mask = jnp.where(upper, mask[:, half_cols:], mask[:, :half_cols])
            return jnp.where((mask != 0)[:, :, None], pairs, jnp.zeros((), BF16))

        t_b = masked(pair_tile, mask_tile, y == 0)
        t_a = masked(*after((pair_tile, mask_tile), t_b), y == 1)
        y_a = send(t_b, TO_Y)
        z_a = send(t_a, TO_Z)
        m_0 = send(t_a, ACROSS)
        gate = out_gate(pair_tile, gain_in, w_out_gate)
        y_b = send(after(t_a, z_a), TO_Y)
        yz_a = send(after(y_a, gate), TO_Z)
        m_1 = send(y_a, ACROSS)
        z_b = send(after(t_b, yz_a), TO_Z)
        yz_b = send(after(z_a, y_b), TO_Y)

        keep = ((z % 2) == c).astype(jnp.int32)[None]
        sets = [((t_a, y_a), (z_a, yz_a)), ((t_b, y_b), (z_b, yz_b))]
        part = half_cols // 2
        a_1 = project(keep, (z_a, yz_a), None, gain_in, w_a, 0, part)
        a_2 = project(keep, (z_a, yz_a), None, gain_in, after(w_a, a_1), part, part)
        got_1, got_2 = send(a_1, ACROSS), send(a_2, ACROSS)
        give_0 = project(1 - keep, *sets[0], gain_in, after(w_b, a_2))
        a_0 = project(inner_flag, (m_0, m_1), (t_a, y_a), gain_in, after(w_a, give_0))
        a_0_sib = send(a_0, TO_CORE)
        keep_0 = project(keep, *sets[0], gain_in, after(w_b, a_0))
        give_1 = project(1 - keep, *sets[1], gain_in, after(w_b, keep_0))
        keep_1 = project(keep, *sets[1], gain_in, after(w_b, give_1))
        b_parts = [keep_0, keep_1, send(give_0, TO_CORE), send(give_1, TO_CORE)]

        done_0 = triangle(inner_flag, [(a_0, a_0_sib)], b_parts, gain_out)
        pair_1 = [(got_1, send(got_1, INNER_CORE)), (a_1, send(a_1, OUTER_CORE))]
        done_1 = triangle(inner_flag, pair_1, b_parts, after(gain_out, done_0))
        pair_2 = [(got_2, send(after(got_2, done_1), INNER_CORE)), (a_2, send(a_2, OUTER_CORE))]
        done_2 = triangle(inner_flag, pair_2, b_parts, after(gain_out, done_1))
        done = (done_0, done_1, done_2)

        got = [[send(v, home(from_y, min(turn, 1))) for turn, v in enumerate(done)] for from_y in (0, 1)]
        block_half = jnp.where(inner, 1 - half, half)
        turn = half ^ c
        own = (block_half == y) & (2 * half + c == z)
        pick = jnp.stack([turn + jnp.where(own & (y == from_y), 2, 0) for from_y in (0, 1)]).astype(jnp.int32)
        out = None
        for q in (0, 1):
            candidates = [(got[s][0], got[s][1 + q], done_0, done[1 + q]) for s in (0, 1)]
            out = finish(pick, pair_tile, gate, candidates, w_out, q, out)
        return out

    return jax.shard_map(local_step, mesh=mesh, in_specs=(tile_spec, mask_spec) + (replicated,) * 8, out_specs=tile_spec, check_vma=False)
```

```python
import math

import jax
import jax.numpy as jnp
from jax import lax
from jax.experimental import pallas as pl
from jax.experimental.pallas import tpu as pltpu
from jax.sharding import PartitionSpec as P


LN_EPS = 0.00001
AXES = ('col', 'row')
BF16, F32 = jnp.bfloat16, jnp.float32
VMEM_BYTES = 60 * 2**20
FLOPS_PER_US = 5_000_000


def moves(target):
    pairs = []
    for z in range(4):
        for y in range(2):
            for c in range(2):
                to = target(y, z, c)
                if to is not None:
                    pairs.append((z * 4 + y * 2 + c, to[1] * 4 + to[0] * 2 + to[2]))
    return pairs


TO_Y = moves(lambda y, z, c: (1 - y, z, c))
TO_Z = moves(lambda y, z, c: (y, z ^ 1, c))
TO_CORE = moves(lambda y, z, c: (y, z, 1 - c))
ACROSS = moves(lambda y, z, c: (y, 3 - z, c) if z in (1, 2) else None)
INNER_CORE = moves(lambda y, z, c: (y, z, 1 - c) if z in (1, 2) else None)
OUTER_CORE = moves(lambda y, z, c: (y, z, 1 - c) if z in (0, 3) else None)


def home(from_y, turn):
    def target(y, z, c):
        if y != from_y:
            return None
        half = z // 2
        block_half = 1 - half if z in (1, 2) else half
        to = (block_half, 2 * half + c, half ^ turn)
        return None if to == (y, z, c) else to

    return moves(target)


def send(value, pairs):
    return lax.ppermute(value, AXES, pairs)


def after(value, *others):
    return lax.optimization_barrier((value,) + others)[0]


def cost(us, nbytes):
    return pl.CostEstimate(flops=us * FLOPS_PER_US, bytes_accessed=nbytes, transcendentals=0)


def params():
    return pltpu.CompilerParams(vmem_limit_bytes=VMEM_BYTES)


def normed(values, gain):
    mean_val = jnp.mean(values, axis=-1, keepdims=True)
    centered = values - mean_val
    variance = jnp.mean(centered * centered, axis=-1, keepdims=True)
    return (centered * lax.rsqrt(variance + LN_EPS) * gain).astype(BF16)


def dot_nt(lhs, rhs):
    return lax.dot_general(lhs, rhs, (((1,), (1,)), ((), ())), preferred_element_type=F32)


def project_body(pieces, gain_ref, w_ref, out_ref, s_ref):
    tri = s_ref.shape[1]
    gain = gain_ref[...].astype(F32)
    x = jnp.concatenate([normed(p.astype(F32), gain) for p in pieces], axis=0)
    x = jnp.swapaxes(x, 0, 1)
    for i in range(x.shape[0]):
        proj = dot_nt(w_ref[...], x[i])
        s_ref[i] = jax.nn.sigmoid(proj[tri:]) * proj[:tri]
    out_ref[...] = jnp.swapaxes(s_ref[...], 0, 1).astype(BF16)


def project_kernel(flag_ref, *refs):
    *piece_refs, gain_ref, w_ref, out_ref, s_ref = refs
    pieces = [ref[...] for ref in piece_refs]
    if len(pieces) == 4:
        pick = flag_ref[0] != 0
        pieces = [jnp.where(pick, yes, no) for yes, no in zip(pieces[:2], pieces[2:])]
    project_body(pieces, gain_ref, w_ref, out_ref, s_ref)


def project(flag, yes, no, gain, w_t, first=0, count=None, blk=16):
    rows, cols, dim = yes[0].shape
    count = count or cols
    blk = min(blk, count)
    wide = w_t.shape[0]
    tri = wide // 2
    at = first // blk
    specs = [pl.BlockSpec((rows, blk, dim), lambda g, f: (0, at + g * f[0], 0) if no else (0, at + g, 0))] * 2
    if no:
        specs += [pl.BlockSpec((rows, blk, dim), lambda g, f: (0, at + g * (1 - f[0]), 0))] * 2
    whole = [pl.BlockSpec((1, dim), lambda g, f: (0, 0)), pl.BlockSpec((wide, dim), lambda g, f: (0, 0))]
    return pl.pallas_call(
        project_kernel,
        grid_spec=pltpu.PrefetchScalarGridSpec(
            num_scalar_prefetch=1,
            grid=(count // blk,),
            in_specs=specs + whole,
            out_specs=pl.BlockSpec((tri, blk, 2 * rows), lambda g, f: (0, g, 0)),
            scratch_shapes=[pltpu.VMEM((blk, tri, 2 * rows), F32)],
        ),
        out_shape=jax.ShapeDtypeStruct((tri, count, 2 * rows), BF16),
        compiler_params=params(),
        cost_estimate=cost(23 * count // cols, 4 * rows * count * (dim + tri)),
        name='project',
    )(flag, *yes, *(no or ()), gain, w_t)


def triangle_kernel(n_pair, n_part, flag_ref, *refs):
    a_refs, b_refs = refs[:2 * n_pair], refs[2 * n_pair:2 * n_pair + 2 * n_part]
    gain_ref, out_ref, *o_refs = refs[2 * n_pair + 2 * n_part:]
    step, steps = pl.program_id(0), pl.num_programs(0)
    n_h, n_i, _ = a_refs[0].shape
    n_j = out_ref.shape[1]
    tri, pitch = n_h * steps, n_i + 8
    spans = [(at, min(128, n_j - at)) for at in range(0, n_j, 128)]
    pick = flag_ref[0] != 0
    for h in range(n_h):
        a_0, a_1 = a_refs[0][h], a_refs[1][h]
        if n_pair == 2:
            a_0, a_1 = jnp.where(pick, a_0, a_refs[2][h]), jnp.where(pick, a_1, a_refs[3][h])
        acc = dot_nt(a_0, jnp.concatenate([ref[h] for ref in b_refs[:n_part]], axis=0))
        acc += dot_nt(a_1, jnp.concatenate([ref[h] for ref in b_refs[n_part:]], axis=0))
        start = pl.multiple_of((step * n_h + h) * pitch, 8)
        for (at, width), o_ref in zip(spans, o_refs):
            o_ref[pl.ds(start, n_i), :width] = acc[:, at:at + width]

    @pl.when(step == steps - 1)
    def _():
        gain = gain_ref[...].astype(F32)

        @pl.loop(0, n_i, step=4)
        def _(first):
            for i in range(4):
                for (at, width), o_ref in zip(spans, o_refs):
                    values = o_ref[pl.ds(first + i, tri, stride=pitch), :][:, :width]
                    mean_val = jnp.mean(values, axis=0, keepdims=True)
                    centered = values - mean_val
                    variance = jnp.mean(centered * centered, axis=0, keepdims=True)
                    unit = centered * lax.rsqrt(variance + LN_EPS)
                    out_ref[first + i, pl.ds(at, width), :] = (unit.T * gain).astype(BF16)


def triangle(flag, a_pairs, b_parts, gain, blk=8):
    n_pair, n_part = len(a_pairs), len(b_parts) // 2
    tri, n_i, n_k = a_pairs[0][0].shape
    part_j = b_parts[0].shape[1]
    n_j = n_part * part_j
    specs = []
    for q in range(n_pair):
        specs += [pl.BlockSpec((blk, n_i, n_k), lambda g, f, q=q: (jnp.where(f[0] == 1 - q, g, 0) if n_pair == 2 else g, 0, 0))] * 2
    return pl.pallas_call(
        lambda *refs: triangle_kernel(n_pair, n_part, *refs),
        grid_spec=pltpu.PrefetchScalarGridSpec(
            num_scalar_prefetch=1,
            grid=(tri // blk,),
            in_specs=specs + [pl.BlockSpec((blk, part_j, n_k), lambda g, f: (g, 0, 0))] * (2 * n_part) + [pl.BlockSpec((1, tri), lambda g, f: (0, 0))],
            out_specs=pl.BlockSpec((n_i, n_j, tri), lambda g, f: (0, 0, 0)),
            scratch_shapes=[pltpu.VMEM((tri * (n_i + 8), 128), F32)] * pl.cdiv(n_j, 128),
        ),
        out_shape=jax.ShapeDtypeStruct((n_i, n_j, tri), BF16),
        compiler_params=params(),
        cost_estimate=cost(40, 2 * tri * n_k * 2 * (n_i + n_j)),
        name='triangle',
    )(flag, *[a for pair in a_pairs for a in pair], *b_parts, gain)


def gate_kernel(z_ref, gain_ref, wg_ref, out_ref):
    rows, cols, dim = z_ref.shape
    x = normed(z_ref[...].astype(F32).reshape(rows * cols, dim), gain_ref[...].astype(F32))
    out_ref[...] = jax.nn.sigmoid(jnp.dot(x, wg_ref[...], preferred_element_type=F32)).reshape(rows, cols, dim)


def out_gate(pair_tile, gain, w_gate, blk=16):
    rows, cols, dim = pair_tile.shape
    blk = min(blk, rows)
    spec = pl.BlockSpec((blk, cols, dim), lambda g: (g, 0, 0))
    return pl.pallas_call(
        gate_kernel,
        grid=(rows // blk,),
        in_specs=[spec, pl.BlockSpec((1, dim), lambda g: (0, 0)), pl.BlockSpec((dim, dim), lambda g: (0, 0))],
        out_specs=spec,
        out_shape=jax.ShapeDtypeStruct(pair_tile.shape, F32),
        compiler_params=params(),
        cost_estimate=cost(18, 6 * rows * cols * dim),
        name='out_gate',
    )(pair_tile, gain, w_gate)


def finish_kernel(sizes, pick_ref, z_ref, gate_ref, *refs):
    wo_ref, out_ref = refs[2 * sum(sizes)], refs[-1]
    rows, cols, dim = z_ref.shape
    half_cols = cols // 2
    for s in (0, 1):
        for q, size in enumerate(sizes):
            first = s * sum(sizes) + sum(sizes[:q])

            @pl.when((pl.program_id(0) == s) & (pick_ref[s] == q))
            def _(s=s, y_refs=refs[first:first + size]):
                @pl.loop(0, rows, step=4)
                def _(r):
                    at = pl.ds(r, 4)
                    for j in (0, 1):
                        to, part = pl.ds(j * half_cols, half_cols), j ^ s
                        y_part = y_refs[part][at] if len(y_refs) == 2 else y_refs[0][at, pl.ds(part * half_cols, half_cols), :]
                        update = jnp.dot(y_part.reshape(4 * half_cols, -1), wo_ref[...], preferred_element_type=F32)
                        total = z_ref[at, to, :].astype(F32) + gate_ref[at, to, :] * update.reshape(4, half_cols, dim)
                        out_ref[at, to, :] = total.astype(BF16)


def finish(pick, pair_tile, gate, candidates, w_out, first, count, so_far=None, blk=16):
    rows, cols, dim = pair_tile.shape
    half_rows = rows // 2
    blk = math.gcd(blk, math.gcd(first, count))
    tri = w_out.shape[0]
    sizes = tuple(len(c) for c in candidates[0])

    def y_spec(half, cand, array):
        skip = first // blk if array.shape[0] == half_rows else 0

        def index(s, g, pick_ref):
            return jnp.where((s == half) & (pick_ref[half] == cand), skip + g, 0), 0, 0

        return pl.BlockSpec((blk, array.shape[1], tri), index)

    tile_spec = pl.BlockSpec((blk, cols, dim), lambda s, g, pick_ref: (s * (half_rows // blk) + first // blk + g, 0, 0))
    y_specs = [y_spec(s, q, v) for s in (0, 1) for q, c in enumerate(candidates[s]) for v in c]
    operands = [pick, pair_tile, gate] + [v for s in (0, 1) for c in candidates[s] for v in c] + [w_out]
    specs = [tile_spec, tile_spec] + y_specs + [pl.BlockSpec(w_out.shape, lambda s, g, pick_ref: (0, 0))]
    aliases = {}
    if so_far is not None:
        aliases = {len(operands): 0}
        operands.append(so_far)
        specs.append(pl.BlockSpec(memory_space=pl.ANY))
    return pl.pallas_call(
        lambda *refs: finish_kernel(sizes, *refs),
        grid_spec=pltpu.PrefetchScalarGridSpec(num_scalar_prefetch=1, grid=(2, count // blk), in_specs=specs, out_specs=tile_spec),
        out_shape=jax.ShapeDtypeStruct(pair_tile.shape, BF16),
        input_output_aliases=aliases,
        compiler_params=params(),
        cost_estimate=cost(8, 5 * rows * cols * dim),
        name='finish',
    )(*operands)


def solution(mesh):
    tile_spec = P(('batch', 'row'), 'col', None)
    mask_spec = P(('batch', 'row'), 'col')
    replicated = P()

    def local_step(pair_tile, mask_tile, ln_in_scale, w_left, w_left_gate, w_right, w_right_gate, w_out_gate, ln_out_scale, w_out):
        _, cols, _ = pair_tile.shape
        half_cols = cols // 2
        row, z = lax.axis_index('row'), lax.axis_index('col')
        y, c = row // 2, row % 2
        half = z // 2
        w_a = jnp.concatenate([w_left, w_left_gate], axis=1).T
        w_b = jnp.concatenate([w_right, w_right_gate], axis=1).T
        gain_in, gain_out = ln_in_scale[None], ln_out_scale[None]

        inner = (z == 1) | (z == 2)
        inner_flag, outer_flag = inner.astype(jnp.int32)[None], (1 - inner.astype(jnp.int32))[None]

        def masked(pairs, mask, upper):
            pairs = jnp.where(upper, pairs[:, half_cols:], pairs[:, :half_cols])
            mask = jnp.where(upper, mask[:, half_cols:], mask[:, :half_cols])
            return jnp.where((mask != 0)[:, :, None], pairs, jnp.zeros((), BF16))

        t_b = masked(pair_tile, mask_tile, y == 0)
        t_a = masked(*after((pair_tile, mask_tile), t_b), y == 1)
        y_a = send(t_b, TO_Y)
        z_a = send(t_a, TO_Z)
        m_0 = send(t_a, ACROSS)
        gate = out_gate(pair_tile, gain_in, w_out_gate)
        y_b = send(after(t_a, z_a), TO_Y)
        yz_a = send(after(y_a, gate), TO_Z)
        m_1 = send(y_a, ACROSS)
        z_b = send(after(t_b, yz_a), TO_Z)
        yz_b = send(after(z_a, y_b), TO_Y)

        keep = ((z % 2) == c).astype(jnp.int32)[None]
        sets = [((t_a, y_a), (z_a, yz_a)), ((t_b, y_b), (z_b, yz_b))]
        big = half_cols * 2 // 3
        small = half_cols - big
        a_1 = project(keep, (z_a, yz_a), None, gain_in, w_a, 0, big)
        a_2 = project(keep, (z_a, yz_a), None, gain_in, after(w_a, a_1), big, small)
        got_1, got_2 = send(a_1, ACROSS), send(a_2, ACROSS)
        give_0 = project(1 - keep, *sets[0], gain_in, after(w_b, a_2))
        a_0 = project(inner_flag, (m_0, m_1), (t_a, y_a), gain_in, after(w_a, give_0))
        a_pair = [(a_0, send(a_0, TO_CORE))]
        keep_0 = project(keep, *sets[0], gain_in, after(w_b, a_0))
        b_0 = [keep_0, send(give_0, TO_CORE)]
        done_0 = triangle(inner_flag, a_pair, b_0, gain_out)
        give_1 = project(1 - keep, *sets[1], gain_in, after(w_b, done_0))
        keep_1 = project(keep, *sets[1], gain_in, after(w_b, give_1))
        b_1 = [keep_1, send(give_1, TO_CORE)]
        b_parts = [b_0[0], b_1[0], b_0[1], b_1[1]]
        done_1 = triangle(inner_flag, a_pair, b_1, gain_out)
        pair_1 = [(got_1, send(got_1, INNER_CORE)), (a_1, send(a_1, OUTER_CORE))]
        done_2 = triangle(inner_flag, pair_1, b_parts, after(gain_out, done_1))
        pair_2 = [(got_2, send(after(got_2, done_2), INNER_CORE)), (a_2, send(a_2, OUTER_CORE))]
        done_3 = triangle(inner_flag, pair_2, b_parts, after(gain_out, done_2))
        done = (done_0, done_1, done_2, done_3)

        got = [[send(v, home(from_y, n // 2)) for n, v in enumerate(done)] for from_y in (0, 1)]
        block_half = jnp.where(inner, 1 - half, half)
        turn = half ^ c
        own = (block_half == y) & (2 * half + c == z)
        pick = jnp.stack([turn + jnp.where(own & (y == from_y), 2, 0) for from_y in (0, 1)]).astype(jnp.int32)
        out = None
        for n, first, count in ((2, 0, big), (3, big, small)):
            candidates = [(tuple(got[s][:2]), (got[s][n],), (done_0, done_1), (done[n],)) for s in (0, 1)]
            out = finish(pick, pair_tile, gate, candidates, w_out, first, count, out)
        return out

    return jax.shard_map(local_step, mesh=mesh, in_specs=(tile_spec, mask_spec) + (replicated,) * 8, out_specs=tile_spec, check_vma=False)
```

```python
import math

import jax
import jax.numpy as jnp
from jax import lax
from jax.experimental import pallas as pl
from jax.experimental.pallas import tpu as pltpu
from jax.sharding import PartitionSpec as P


LN_EPS = 0.00001
AXES = ('col', 'row')
BF16, F32 = jnp.bfloat16, jnp.float32
VMEM_BYTES = 60 * 2**20
FLOPS_PER_US = 5_000_000


def moves(target):
    pairs = []
    for z in range(4):
        for y in range(2):
            for c in range(2):
                to = target(y, z, c)
                if to is not None:
                    pairs.append((z * 4 + y * 2 + c, to[1] * 4 + to[0] * 2 + to[2]))
    return pairs


TO_Y = moves(lambda y, z, c: (1 - y, z, c))
TO_Z = moves(lambda y, z, c: (y, z ^ 1, c))
TO_CORE = moves(lambda y, z, c: (y, z, 1 - c))
ACROSS = moves(lambda y, z, c: (y, 3 - z, c) if z in (1, 2) else None)
INNER_CORE = moves(lambda y, z, c: (y, z, 1 - c) if z in (1, 2) else None)
OUTER_CORE = moves(lambda y, z, c: (y, z, 1 - c) if z in (0, 3) else None)


def home(from_y, turn):
    def target(y, z, c):
        if y != from_y:
            return None
        half = z // 2
        block_half = 1 - half if z in (1, 2) else half
        to = (block_half, 2 * half + c, half ^ turn)
        return None if to == (y, z, c) else to

    return moves(target)


def send(value, pairs):
    return lax.ppermute(value, AXES, pairs)


def after(value, *others):
    return lax.optimization_barrier((value,) + others)[0]


def cost(us, nbytes):
    return pl.CostEstimate(flops=us * FLOPS_PER_US, bytes_accessed=nbytes, transcendentals=0)


def params():
    return pltpu.CompilerParams(vmem_limit_bytes=VMEM_BYTES)


def normed(values, gain):
    mean_val = jnp.mean(values, axis=-1, keepdims=True)
    centered = values - mean_val
    variance = jnp.mean(centered * centered, axis=-1, keepdims=True)
    return (centered * lax.rsqrt(variance + LN_EPS) * gain).astype(BF16)


def dot_nt(lhs, rhs):
    return lax.dot_general(lhs, rhs, (((1,), (1,)), ((), ())), preferred_element_type=F32)


def prepare(pieces, gain_ref):
    gain = gain_ref[...].astype(F32)
    x = jnp.concatenate([normed(p.astype(F32), gain) for p in pieces], axis=0)
    return jnp.swapaxes(x, 0, 1)


def project_body(x, w_ref, out_ref, s_ref):
    tri = s_ref.shape[1]
    for i in range(x.shape[0]):
        proj = dot_nt(w_ref[...], x[i])
        s_ref[i] = jax.nn.sigmoid(proj[tri:]) * proj[:tri]
    out_ref[...] = jnp.swapaxes(s_ref[...], 0, 1).astype(BF16)


def norm_kernel(p0_ref, p1_ref, gain_ref, x_ref):
    x_ref[...] = prepare((p0_ref[...], p1_ref[...]), gain_ref)


def norm(pieces, gain, blk=16):
    rows, cols, dim = pieces[0].shape
    return pl.pallas_call(
        norm_kernel,
        grid=(cols // blk,),
        in_specs=[pl.BlockSpec((rows, blk, dim), lambda g: (0, g, 0))] * 2 + [pl.BlockSpec((1, dim), lambda g: (0, 0))],
        out_specs=pl.BlockSpec((blk, 2 * rows, dim), lambda g: (g, 0, 0)),
        out_shape=jax.ShapeDtypeStruct((cols, 2 * rows, dim), BF16),
        compiler_params=params(),
        cost_estimate=cost(12, 8 * rows * cols * dim),
        name='norm',
    )(*pieces, gain)


def project_kernel(n_piece, flag_ref, *refs):
    piece_refs, (gain_ref, w_ref, out_ref, *x_refs, s_ref) = refs[:n_piece], refs[n_piece:]
    pieces = [ref[...] for ref in piece_refs]
    if len(pieces) == 4:
        pick = flag_ref[0] != 0
        pieces = [jnp.where(pick, yes, no) for yes, no in zip(pieces[:2], pieces[2:])]
    x = prepare(pieces, gain_ref)
    for x_ref in x_refs:
        x_ref[...] = x
    project_body(x, w_ref, out_ref, s_ref)


def project(flag, yes, no, gain, w_t, first=0, count=None, blk=16, with_x=False):
    rows, cols, dim = yes[0].shape
    count = count or cols
    blk = min(blk, count)
    wide = w_t.shape[0]
    tri = wide // 2
    at = first // blk
    specs = [pl.BlockSpec((rows, blk, dim), lambda g, f: (0, at + g * f[0], 0) if no else (0, at + g, 0))] * 2
    if no:
        specs += [pl.BlockSpec((rows, blk, dim), lambda g, f: (0, at + g * (1 - f[0]), 0))] * 2
    whole = [pl.BlockSpec((1, dim), lambda g, f: (0, 0)), pl.BlockSpec((wide, dim), lambda g, f: (0, 0))]
    out_specs = [pl.BlockSpec((tri, blk, 2 * rows), lambda g, f: (0, g, 0)), pl.BlockSpec((blk, 2 * rows, dim), lambda g, f: (g, 0, 0))]
    out_shape = [jax.ShapeDtypeStruct((tri, count, 2 * rows), BF16), jax.ShapeDtypeStruct((count, 2 * rows, dim), BF16)]
    n_piece, n_out = len(specs), 2 if with_x else 1
    out = pl.pallas_call(
        lambda *refs: project_kernel(n_piece, *refs),
        grid_spec=pltpu.PrefetchScalarGridSpec(
            num_scalar_prefetch=1,
            grid=(count // blk,),
            in_specs=specs + whole,
            out_specs=out_specs[:n_out],
            scratch_shapes=[pltpu.VMEM((blk, tri, 2 * rows), F32)],
        ),
        out_shape=out_shape[:n_out],
        compiler_params=params(),
        cost_estimate=cost(23 * count // cols, 4 * rows * count * (dim + tri)),
        name='project',
    )(flag, *yes, *(no or ()), gain, w_t)
    return out if with_x else out[0]


def project_x_kernel(n_first, flag_ref, yes_ref, no0_ref, no1_ref, w_ref, out_ref, s_ref):
    no = jnp.where(pl.program_id(0) < n_first, no0_ref[...], no1_ref[...])
    project_body(jnp.where(flag_ref[0] != 0, yes_ref[...], no), w_ref, out_ref, s_ref)


def project_x(flag, yes, no, w_t, blk=16):
    cols, deep, dim = yes.shape
    wide = w_t.shape[0]
    tri = wide // 2
    blk = math.gcd(blk, math.gcd(no[0].shape[0], no[1].shape[0]))
    n_first = no[0].shape[0] // blk
    return pl.pallas_call(
        lambda *refs: project_x_kernel(n_first, *refs),
        grid_spec=pltpu.PrefetchScalarGridSpec(
            num_scalar_prefetch=1,
            grid=(cols // blk,),
            in_specs=[
                pl.BlockSpec((blk, deep, dim), lambda g, f: (g * f[0], 0, 0)),
                pl.BlockSpec((blk, deep, dim), lambda g, f: (jnp.minimum(g, n_first - 1) * (1 - f[0]), 0, 0)),
                pl.BlockSpec((blk, deep, dim), lambda g, f: (jnp.maximum(g - n_first, 0) * (1 - f[0]), 0, 0)),
                pl.BlockSpec((wide, dim), lambda g, f: (0, 0)),
            ],
            out_specs=pl.BlockSpec((tri, blk, deep), lambda g, f: (0, g, 0)),
            scratch_shapes=[pltpu.VMEM((blk, tri, deep), F32)],
        ),
        out_shape=jax.ShapeDtypeStruct((tri, cols, deep), BF16),
        compiler_params=params(),
        cost_estimate=cost(14, 2 * cols * deep * (dim + tri)),
        name='project_x',
    )(flag, yes, *no, w_t)


def triangle_kernel(n_pair, n_part, flag_ref, *refs):
    a_refs, b_refs = refs[:2 * n_pair], refs[2 * n_pair:2 * n_pair + 2 * n_part]
    gain_ref, out_ref, *o_refs = refs[2 * n_pair + 2 * n_part:]
    step, steps = pl.program_id(0), pl.num_programs(0)
    n_h, n_i, _ = a_refs[0].shape
    n_j = out_ref.shape[1]
    tri, pitch = n_h * steps, n_i + 8
    spans = [(at, min(128, n_j - at)) for at in range(0, n_j, 128)]
    pick = flag_ref[0] != 0

    @pl.loop(0, n_h, step=8)
    def _(group):
        for k in range(8):
            h = group + k
            a_0, a_1 = a_refs[0][h], a_refs[1][h]
            if n_pair == 2:
                a_0, a_1 = jnp.where(pick, a_0, a_refs[2][h]), jnp.where(pick, a_1, a_refs[3][h])
            acc = dot_nt(a_0, jnp.concatenate([ref[h] for ref in b_refs[:n_part]], axis=0))
            acc += dot_nt(a_1, jnp.concatenate([ref[h] for ref in b_refs[n_part:]], axis=0))
            start = pl.multiple_of((step * n_h + h) * pitch, 8)
            for (at, width), o_ref in zip(spans, o_refs):
                o_ref[pl.ds(start, n_i), :width] = acc[:, at:at + width]

    @pl.when(step == steps - 1)
    def _():
        gain = gain_ref[...].astype(F32)

        @pl.loop(0, n_i, step=4)
        def _(first):
            for i in range(4):
                for (at, width), o_ref in zip(spans, o_refs):
                    values = o_ref[pl.ds(first + i, tri, stride=pitch), :][:, :width]
                    mean_val = jnp.mean(values, axis=0, keepdims=True)
                    centered = values - mean_val
                    variance = jnp.mean(centered * centered, axis=0, keepdims=True)
                    unit = centered * lax.rsqrt(variance + LN_EPS)
                    out_ref[first + i, pl.ds(at, width), :] = (unit.T * gain).astype(BF16)


def triangle(flag, a_pairs, b_parts, gain, blk=16):
    n_pair, n_part = len(a_pairs), len(b_parts) // 2
    tri, n_i, n_k = a_pairs[0][0].shape
    part_j = b_parts[0].shape[1]
    n_j = n_part * part_j
    specs = []
    for q in range(n_pair):
        specs += [pl.BlockSpec((blk, n_i, n_k), lambda g, f, q=q: (jnp.where(f[0] == 1 - q, g, 0) if n_pair == 2 else g, 0, 0))] * 2
    return pl.pallas_call(
        lambda *refs: triangle_kernel(n_pair, n_part, *refs),
        grid_spec=pltpu.PrefetchScalarGridSpec(
            num_scalar_prefetch=1,
            grid=(tri // blk,),
            in_specs=specs + [pl.BlockSpec((blk, part_j, n_k), lambda g, f: (g, 0, 0))] * (2 * n_part) + [pl.BlockSpec((1, tri), lambda g, f: (0, 0))],
            out_specs=pl.BlockSpec((n_i, n_j, tri), lambda g, f: (0, 0, 0)),
            scratch_shapes=[pltpu.VMEM((tri * (n_i + 8), 128), F32)] * pl.cdiv(n_j, 128),
        ),
        out_shape=jax.ShapeDtypeStruct((n_i, n_j, tri), BF16),
        compiler_params=params(),
        cost_estimate=cost(40, 2 * tri * n_k * 2 * (n_i + n_j)),
        name='triangle',
    )(flag, *[a for pair in a_pairs for a in pair], *b_parts, gain)


def gate_kernel(z_ref, gain_ref, wg_ref, out_ref):
    rows, cols, dim = z_ref.shape
    x = normed(z_ref[...].astype(F32).reshape(rows * cols, dim), gain_ref[...].astype(F32))
    out_ref[...] = jax.nn.sigmoid(jnp.dot(x, wg_ref[...], preferred_element_type=F32)).reshape(rows, cols, dim)


def out_gate(pair_tile, gain, w_gate, blk=16):
    rows, cols, dim = pair_tile.shape
    blk = min(blk, rows)
    spec = pl.BlockSpec((blk, cols, dim), lambda g: (g, 0, 0))
    return pl.pallas_call(
        gate_kernel,
        grid=(rows // blk,),
        in_specs=[spec, pl.BlockSpec((1, dim), lambda g: (0, 0)), pl.BlockSpec((dim, dim), lambda g: (0, 0))],
        out_specs=spec,
        out_shape=jax.ShapeDtypeStruct(pair_tile.shape, F32),
        compiler_params=params(),
        cost_estimate=cost(18, 6 * rows * cols * dim),
        name='out_gate',
    )(pair_tile, gain, w_gate)


def finish_kernel(sizes, pick_ref, z_ref, gate_ref, *refs):
    wo_ref, out_ref = refs[2 * sum(sizes)], refs[-1]
    rows, cols, dim = z_ref.shape
    half_cols = cols // 2
    for s in (0, 1):
        for q, size in enumerate(sizes):
            first = s * sum(sizes) + sum(sizes[:q])

            @pl.when((pl.program_id(0) == s) & (pick_ref[s] == q))
            def _(s=s, y_refs=refs[first:first + size]):
                @pl.loop(0, rows, step=4)
                def _(r):
                    at = pl.ds(r, 4)
                    for j in (0, 1):
                        to, part = pl.ds(j * half_cols, half_cols), j ^ s
                        y_part = y_refs[part][at] if len(y_refs) == 2 else y_refs[0][at, pl.ds(part * half_cols, half_cols), :]
                        update = jnp.dot(y_part.reshape(4 * half_cols, -1), wo_ref[...], preferred_element_type=F32)
                        total = z_ref[at, to, :].astype(F32) + gate_ref[at, to, :] * update.reshape(4, half_cols, dim)
                        out_ref[at, to, :] = total.astype(BF16)


def finish(pick, pair_tile, gate, candidates, w_out, first, count, so_far=None, blk=16):
    rows, cols, dim = pair_tile.shape
    half_rows = rows // 2
    blk = math.gcd(blk, math.gcd(first, count))
    tri = w_out.shape[0]
    sizes = tuple(len(c) for c in candidates[0])

    def y_spec(half, cand, array):
        skip = first // blk if array.shape[0] == half_rows else 0

        def index(s, g, pick_ref):
            return jnp.where((s == half) & (pick_ref[half] == cand), skip + g, 0), 0, 0

        return pl.BlockSpec((blk, array.shape[1], tri), index)

    tile_spec = pl.BlockSpec((blk, cols, dim), lambda s, g, pick_ref: (s * (half_rows // blk) + first // blk + g, 0, 0))
    y_specs = [y_spec(s, q, v) for s in (0, 1) for q, c in enumerate(candidates[s]) for v in c]
    operands = [pick, pair_tile, gate] + [v for s in (0, 1) for c in candidates[s] for v in c] + [w_out]
    specs = [tile_spec, tile_spec] + y_specs + [pl.BlockSpec(w_out.shape, lambda s, g, pick_ref: (0, 0))]
    aliases = {}
    if so_far is not None:
        aliases = {len(operands): 0}
        operands.append(so_far)
        specs.append(pl.BlockSpec(memory_space=pl.ANY))
    return pl.pallas_call(
        lambda *refs: finish_kernel(sizes, *refs),
        grid_spec=pltpu.PrefetchScalarGridSpec(num_scalar_prefetch=1, grid=(2, count // blk), in_specs=specs, out_specs=tile_spec),
        out_shape=jax.ShapeDtypeStruct(pair_tile.shape, BF16),
        input_output_aliases=aliases,
        compiler_params=params(),
        cost_estimate=cost(8, 5 * rows * cols * dim),
        name='finish',
    )(*operands)


def solution(mesh):
    tile_spec = P(('batch', 'row'), 'col', None)
    mask_spec = P(('batch', 'row'), 'col')
    replicated = P()

    def local_step(pair_tile, mask_tile, ln_in_scale, w_left, w_left_gate, w_right, w_right_gate, w_out_gate, ln_out_scale, w_out):
        _, cols, _ = pair_tile.shape
        half_cols = cols // 2
        row, z = lax.axis_index('row'), lax.axis_index('col')
        y, c = row // 2, row % 2
        half = z // 2
        w_a = jnp.concatenate([w_left, w_left_gate], axis=1).T
        w_b = jnp.concatenate([w_right, w_right_gate], axis=1).T
        gain_in, gain_out = ln_in_scale[None], ln_out_scale[None]

        inner = (z == 1) | (z == 2)
        inner_flag, outer_flag = inner.astype(jnp.int32)[None], (1 - inner.astype(jnp.int32))[None]

        def masked(pairs, mask, upper):
            pairs = jnp.where(upper, pairs[:, half_cols:], pairs[:, :half_cols])
            mask = jnp.where(upper, mask[:, half_cols:], mask[:, :half_cols])
            return jnp.where((mask != 0)[:, :, None], pairs, jnp.zeros((), BF16))

        t_b = masked(pair_tile, mask_tile, y == 0)
        t_a = masked(*after((pair_tile, mask_tile), t_b), y == 1)
        y_a = send(t_b, TO_Y)
        z_a = send(t_a, TO_Z)
        m_0 = send(t_a, ACROSS)
        gate = out_gate(pair_tile, gain_in, w_out_gate)
        y_b = send(after(t_a, z_a), TO_Y)
        yz_a = send(after(y_a, gate), TO_Z)
        m_1 = send(y_a, ACROSS)
        z_b = send(after(t_b, yz_a), TO_Z)
        yz_b = send(after(z_a, y_b), TO_Y)

        keep = ((z % 2) == c).astype(jnp.int32)[None]
        seconds = (t_b, y_b), (z_b, yz_b)
        big = half_cols * 2 // 3
        small = half_cols - big
        x_own = norm((t_a, y_a), gain_in)
        a_1, x_1 = project(keep, (z_a, yz_a), None, gain_in, after(w_a, x_own), 0, big, with_x=True)
        a_2, x_2 = project(keep, (z_a, yz_a), None, gain_in, after(w_a, a_1), big, small, with_x=True)
        got_1, got_2 = send(a_1, ACROSS), send(a_2, ACROSS)
        give_0 = project_x(1 - keep, x_own, (x_1, x_2), after(w_b, a_2))
        a_0 = project(inner_flag, (m_0, m_1), (t_a, y_a), gain_in, after(w_a, give_0))
        a_pair = [(a_0, send(a_0, TO_CORE))]
        keep_0 = project_x(keep, x_own, (x_1, x_2), after(w_b, a_0))
        b_0 = [keep_0, send(give_0, TO_CORE)]
        done_0 = triangle(inner_flag, a_pair, b_0, gain_out)
        give_1 = project(1 - keep, *seconds, gain_in, after(w_b, done_0))
        keep_1 = project(keep, *seconds, gain_in, after(w_b, give_1))
        b_1 = [keep_1, send(give_1, TO_CORE)]
        b_parts = [b_0[0], b_1[0], b_0[1], b_1[1]]
        done_1 = triangle(inner_flag, a_pair, b_1, gain_out)
        pair_1 = [(got_1, send(after(got_1, keep_1), INNER_CORE)), (a_1, send(a_1, OUTER_CORE))]
        done_2 = triangle(inner_flag, pair_1, b_parts, after(gain_out, done_1))
        pair_2 = [(got_2, send(after(got_2, done_2), INNER_CORE)), (a_2, send(a_2, OUTER_CORE))]
        done_3 = triangle(inner_flag, pair_2, b_parts, after(gain_out, done_2))
        done = (done_0, done_1, done_2, done_3)

        got = [[send(v, home(from_y, n // 2)) for n, v in enumerate(done)] for from_y in (0, 1)]
        block_half = jnp.where(inner, 1 - half, half)
        turn = half ^ c
        own = (block_half == y) & (2 * half + c == z)
        pick = jnp.stack([turn + jnp.where(own & (y == from_y), 2, 0) for from_y in (0, 1)]).astype(jnp.int32)
        out = None
        for n, first, count in ((2, 0, big), (3, big, small)):
            candidates = [(tuple(got[s][:2]), (got[s][n],), (done_0, done_1), (done[n],)) for s in (0, 1)]
            out = finish(pick, pair_tile, gate, candidates, w_out, first, count, out)
        return out

    return jax.shard_map(local_step, mesh=mesh, in_specs=(tile_spec, mask_spec) + (replicated,) * 8, out_specs=tile_spec, check_vma=False)
```

```python
import math

import jax
import jax.numpy as jnp
from jax import lax
from jax.experimental import pallas as pl
from jax.experimental.pallas import tpu as pltpu
from jax.sharding import PartitionSpec as P


LN_EPS = 0.00001
AXES = ('col', 'row')
BF16, F32 = jnp.bfloat16, jnp.float32
VMEM_BYTES = 60 * 2**20
FLOPS_PER_US = 5_000_000


def moves(target):
    pairs = []
    for z in range(4):
        for y in range(2):
            for c in range(2):
                to = target(y, z, c)
                if to is not None:
                    pairs.append((z * 4 + y * 2 + c, to[1] * 4 + to[0] * 2 + to[2]))
    return pairs


TO_Y = moves(lambda y, z, c: (1 - y, z, c))
TO_Z = moves(lambda y, z, c: (y, z ^ 1, c))
TO_CORE = moves(lambda y, z, c: (y, z, 1 - c))
ACROSS = moves(lambda y, z, c: (y, 3 - z, c) if z in (1, 2) else None)
INNER_CORE = moves(lambda y, z, c: (y, z, 1 - c) if z in (1, 2) else None)
OUTER_CORE = moves(lambda y, z, c: (y, z, 1 - c) if z in (0, 3) else None)


def home(from_y, turn):
    def target(y, z, c):
        if y != from_y:
            return None
        half = z // 2
        block_half = 1 - half if z in (1, 2) else half
        to = (block_half, 2 * half + c, half ^ turn)
        return None if to == (y, z, c) else to

    return moves(target)


def send(value, pairs):
    return lax.ppermute(value, AXES, pairs)


def after(value, *others):
    return lax.optimization_barrier((value,) + others)[0]


def cost(us, nbytes):
    return pl.CostEstimate(flops=us * FLOPS_PER_US, bytes_accessed=nbytes, transcendentals=0)


def params():
    return pltpu.CompilerParams(vmem_limit_bytes=VMEM_BYTES)


def normed(values, gain):
    mean_val = jnp.mean(values, axis=-1, keepdims=True)
    centered = values - mean_val
    variance = jnp.mean(centered * centered, axis=-1, keepdims=True)
    return (centered * lax.rsqrt(variance + LN_EPS) * gain).astype(BF16)


def dot_nt(lhs, rhs):
    return lax.dot_general(lhs, rhs, (((1,), (1,)), ((), ())), preferred_element_type=F32)


def prepare(pieces, gain_ref):
    gain = gain_ref[...].astype(F32)
    x = jnp.concatenate([normed(p.astype(F32), gain) for p in pieces], axis=0)
    return jnp.swapaxes(x, 0, 1)


def project_body(x, w_ref, out_ref, s_ref):
    tri = s_ref.shape[1]
    for i in range(x.shape[0]):
        proj = dot_nt(w_ref[...], x[i])
        s_ref[i] = jax.nn.sigmoid(proj[tri:]) * proj[:tri]
    out_ref[...] = jnp.swapaxes(s_ref[...], 0, 1).astype(BF16)


def norm_kernel(p0_ref, p1_ref, gain_ref, x_ref):
    x_ref[...] = prepare((p0_ref[...], p1_ref[...]), gain_ref)


def norm(pieces, gain, blk=16):
    rows, cols, dim = pieces[0].shape
    return pl.pallas_call(
        norm_kernel,
        grid=(cols // blk,),
        in_specs=[pl.BlockSpec((rows, blk, dim), lambda g: (0, g, 0))] * 2 + [pl.BlockSpec((1, dim), lambda g: (0, 0))],
        out_specs=pl.BlockSpec((blk, 2 * rows, dim), lambda g: (g, 0, 0)),
        out_shape=jax.ShapeDtypeStruct((cols, 2 * rows, dim), BF16),
        compiler_params=params(),
        cost_estimate=cost(12, 8 * rows * cols * dim),
        name='norm',
    )(*pieces, gain)


def project_kernel(n_piece, flag_ref, *refs):
    piece_refs, (gain_ref, w_ref, out_ref, *x_refs, s_ref) = refs[:n_piece], refs[n_piece:]
    pieces = [ref[...] for ref in piece_refs]
    if len(pieces) == 4:
        pick = flag_ref[0] != 0
        pieces = [jnp.where(pick, yes, no) for yes, no in zip(pieces[:2], pieces[2:])]
    x = prepare(pieces, gain_ref)
    for x_ref in x_refs:
        x_ref[...] = x
    project_body(x, w_ref, out_ref, s_ref)


def project(flag, yes, no, gain, w_t, first=0, count=None, blk=16, with_x=False):
    rows, cols, dim = yes[0].shape
    count = count or cols
    blk = min(blk, count)
    wide = w_t.shape[0]
    tri = wide // 2
    at = first // blk
    specs = [pl.BlockSpec((rows, blk, dim), lambda g, f: (0, at + g * f[0], 0) if no else (0, at + g, 0))] * 2
    if no:
        specs += [pl.BlockSpec((rows, blk, dim), lambda g, f: (0, at + g * (1 - f[0]), 0))] * 2
    whole = [pl.BlockSpec((1, dim), lambda g, f: (0, 0)), pl.BlockSpec((wide, dim), lambda g, f: (0, 0))]
    out_specs = [pl.BlockSpec((tri, blk, 2 * rows), lambda g, f: (0, g, 0)), pl.BlockSpec((blk, 2 * rows, dim), lambda g, f: (g, 0, 0))]
    out_shape = [jax.ShapeDtypeStruct((tri, count, 2 * rows), BF16), jax.ShapeDtypeStruct((count, 2 * rows, dim), BF16)]
    n_piece, n_out = len(specs), 2 if with_x else 1
    out = pl.pallas_call(
        lambda *refs: project_kernel(n_piece, *refs),
        grid_spec=pltpu.PrefetchScalarGridSpec(
            num_scalar_prefetch=1,
            grid=(count // blk,),
            in_specs=specs + whole,
            out_specs=out_specs[:n_out],
            scratch_shapes=[pltpu.VMEM((blk, tri, 2 * rows), F32)],
        ),
        out_shape=out_shape[:n_out],
        compiler_params=params(),
        cost_estimate=cost(23 * count // cols, 4 * rows * count * (dim + tri)),
        name='project',
    )(flag, *yes, *(no or ()), gain, w_t)
    return out if with_x else out[0]


def project_x_kernel(n_first, flag_ref, yes_ref, no0_ref, no1_ref, w_ref, out_ref, s_ref):
    no = jnp.where(pl.program_id(0) < n_first, no0_ref[...], no1_ref[...])
    project_body(jnp.where(flag_ref[0] != 0, yes_ref[...], no), w_ref, out_ref, s_ref)


def project_x(flag, yes, no, w_t, blk=16):
    cols, deep, dim = yes.shape
    wide = w_t.shape[0]
    tri = wide // 2
    blk = math.gcd(blk, math.gcd(no[0].shape[0], no[1].shape[0]))
    n_first = no[0].shape[0] // blk
    return pl.pallas_call(
        lambda *refs: project_x_kernel(n_first, *refs),
        grid_spec=pltpu.PrefetchScalarGridSpec(
            num_scalar_prefetch=1,
            grid=(cols // blk,),
            in_specs=[
                pl.BlockSpec((blk, deep, dim), lambda g, f: (g * f[0], 0, 0)),
                pl.BlockSpec((blk, deep, dim), lambda g, f: (jnp.minimum(g, n_first - 1) * (1 - f[0]), 0, 0)),
                pl.BlockSpec((blk, deep, dim), lambda g, f: (jnp.maximum(g - n_first, 0) * (1 - f[0]), 0, 0)),
                pl.BlockSpec((wide, dim), lambda g, f: (0, 0)),
            ],
            out_specs=pl.BlockSpec((tri, blk, deep), lambda g, f: (0, g, 0)),
            scratch_shapes=[pltpu.VMEM((blk, tri, deep), F32)],
        ),
        out_shape=jax.ShapeDtypeStruct((tri, cols, deep), BF16),
        compiler_params=params(),
        cost_estimate=cost(14, 2 * cols * deep * (dim + tri)),
        name='project_x',
    )(flag, yes, *no, w_t)


def triangle_kernel(n_pair, n_part, flag_ref, *refs):
    a_refs, b_refs = refs[:2 * n_pair], refs[2 * n_pair:2 * n_pair + 2 * n_part]
    gain_ref, out_ref, *o_refs = refs[2 * n_pair + 2 * n_part:]
    step, steps = pl.program_id(0), pl.num_programs(0)
    n_h, n_i, _ = a_refs[0].shape
    n_j = out_ref.shape[1]
    tri, pitch = n_h * steps, n_i + 8
    spans = [(at, min(128, n_j - at)) for at in range(0, n_j, 128)]
    pick = flag_ref[0] != 0

    @pl.loop(0, n_h, step=8)
    def _(group):
        for k in range(8):
            h = group + k
            a_0, a_1 = a_refs[0][h], a_refs[1][h]
            if n_pair == 2:
                a_0, a_1 = jnp.where(pick, a_0, a_refs[2][h]), jnp.where(pick, a_1, a_refs[3][h])
            acc = dot_nt(a_0, jnp.concatenate([ref[h] for ref in b_refs[:n_part]], axis=0))
            acc += dot_nt(a_1, jnp.concatenate([ref[h] for ref in b_refs[n_part:]], axis=0))
            start = pl.multiple_of((step * n_h + h) * pitch, 8)
            for (at, width), o_ref in zip(spans, o_refs):
                o_ref[pl.ds(start, n_i), :width] = acc[:, at:at + width]

    @pl.when(step == steps - 1)
    def _():
        gain = gain_ref[...].astype(F32)

        @pl.loop(0, n_i, step=4)
        def _(first):
            for i in range(4):
                for (at, width), o_ref in zip(spans, o_refs):
                    values = o_ref[pl.ds(first + i, tri, stride=pitch), :][:, :width]
                    mean_val = jnp.mean(values, axis=0, keepdims=True)
                    centered = values - mean_val
                    variance = jnp.mean(centered * centered, axis=0, keepdims=True)
                    unit = centered * lax.rsqrt(variance + LN_EPS)
                    out_ref[first + i, pl.ds(at, width), :] = (unit.T * gain).astype(BF16)


def triangle(flag, a_pairs, b_parts, gain, blk=16):
    n_pair, n_part = len(a_pairs), len(b_parts) // 2
    tri, n_i, n_k = a_pairs[0][0].shape
    part_j = b_parts[0].shape[1]
    n_j = n_part * part_j
    specs = []
    for q in range(n_pair):
        specs += [pl.BlockSpec((blk, n_i, n_k), lambda g, f, q=q: (jnp.where(f[0] == 1 - q, g, 0) if n_pair == 2 else g, 0, 0))] * 2
    return pl.pallas_call(
        lambda *refs: triangle_kernel(n_pair, n_part, *refs),
        grid_spec=pltpu.PrefetchScalarGridSpec(
            num_scalar_prefetch=1,
            grid=(tri // blk,),
            in_specs=specs + [pl.BlockSpec((blk, part_j, n_k), lambda g, f: (g, 0, 0))] * (2 * n_part) + [pl.BlockSpec((1, tri), lambda g, f: (0, 0))],
            out_specs=pl.BlockSpec((n_i, n_j, tri), lambda g, f: (0, 0, 0)),
            scratch_shapes=[pltpu.VMEM((tri * (n_i + 8), 128), F32)] * pl.cdiv(n_j, 128),
        ),
        out_shape=jax.ShapeDtypeStruct((n_i, n_j, tri), BF16),
        compiler_params=params(),
        cost_estimate=cost(40, 2 * tri * n_k * 2 * (n_i + n_j)),
        name='triangle',
    )(flag, *[a for pair in a_pairs for a in pair], *b_parts, gain)


def gate_in_kernel(z_ref, gain_ref, out_ref):
    rows, cols, dim = z_ref.shape
    out_ref[...] = normed(z_ref[...].astype(F32).reshape(rows * cols, dim), gain_ref[...].astype(F32)).reshape(rows, cols, dim)


def gate_in(pair_tile, gain, blk=16):
    rows, cols, dim = pair_tile.shape
    blk = min(blk, rows)
    spec = pl.BlockSpec((blk, cols, dim), lambda g: (g, 0, 0))
    return pl.pallas_call(
        gate_in_kernel,
        grid=(rows // blk,),
        in_specs=[spec, pl.BlockSpec((1, dim), lambda g: (0, 0))],
        out_specs=spec,
        out_shape=jax.ShapeDtypeStruct(pair_tile.shape, BF16),
        compiler_params=params(),
        cost_estimate=cost(15, 4 * rows * cols * dim),
        name='gate_in',
    )(pair_tile, gain)


def finish_kernel(sizes, pick_ref, z_ref, x_ref, *refs):
    wo_ref, wg_ref, out_ref = refs[2 * sum(sizes)], refs[2 * sum(sizes) + 1], refs[-2]
    y_ref = refs[-1]
    rows, cols, dim = z_ref.shape
    half_cols = cols // 2
    for s in (0, 1):
        for q, size in enumerate(sizes):
            first = s * sum(sizes) + sum(sizes[:q])

            @pl.when((pl.program_id(0) == s) & (pick_ref[s] == q))
            def _(s=s, y_refs=refs[first:first + size]):
                for j in (0, 1):
                    to, part = pl.ds(j * half_cols, half_cols), j ^ s
                    y_ref[:, to, :] = y_refs[part][...] if len(y_refs) == 2 else y_refs[0][:, pl.ds(part * half_cols, half_cols), :]

    @pl.loop(0, rows, step=8)
    def _(r):
        at, deep = pl.ds(r, 8), 8 * cols
        update = jnp.dot(y_ref[at].reshape(deep, -1), wo_ref[...], preferred_element_type=F32)
        gate = jax.nn.sigmoid(jnp.dot(x_ref[at].reshape(deep, dim), wg_ref[...], preferred_element_type=F32))
        total = z_ref[at].astype(F32).reshape(deep, dim) + gate * update
        out_ref[at] = total.astype(BF16).reshape(8, cols, dim)


def finish(pick, pair_tile, x, candidates, w_out, w_gate, first, count, so_far=None, blk=16):
    rows, cols, dim = pair_tile.shape
    half_rows = rows // 2
    blk = math.gcd(blk, math.gcd(first, count))
    tri = w_out.shape[0]
    sizes = tuple(len(c) for c in candidates[0])

    def y_spec(half, cand, array):
        skip = first // blk if array.shape[0] == half_rows else 0

        def index(s, g, pick_ref):
            return jnp.where((s == half) & (pick_ref[half] == cand), skip + g, 0), 0, 0

        return pl.BlockSpec((blk, array.shape[1], tri), index)

    tile_spec = pl.BlockSpec((blk, cols, dim), lambda s, g, pick_ref: (s * (half_rows // blk) + first // blk + g, 0, 0))
    y_specs = [y_spec(s, q, v) for s in (0, 1) for q, c in enumerate(candidates[s]) for v in c]
    operands = [pick, pair_tile, x] + [v for s in (0, 1) for c in candidates[s] for v in c] + [w_out, w_gate]
    specs = [tile_spec, tile_spec] + y_specs + [pl.BlockSpec(w.shape, lambda s, g, pick_ref: (0, 0)) for w in (w_out, w_gate)]
    aliases = {}
    if so_far is not None:
        aliases = {len(operands): 0}
        operands.append(so_far)
        specs.append(pl.BlockSpec(memory_space=pl.ANY))
    return pl.pallas_call(
        lambda *refs: finish_kernel(sizes, *refs),
        grid_spec=pltpu.PrefetchScalarGridSpec(num_scalar_prefetch=1, grid=(2, count // blk), in_specs=specs, out_specs=tile_spec,
                                              scratch_shapes=[pltpu.VMEM((blk, cols, tri), BF16)]),
        out_shape=jax.ShapeDtypeStruct(pair_tile.shape, BF16),
        input_output_aliases=aliases,
        compiler_params=params(),
        cost_estimate=cost(8, 5 * rows * cols * dim),
        name='finish',
    )(*operands)


def solution(mesh):
    tile_spec = P(('batch', 'row'), 'col', None)
    mask_spec = P(('batch', 'row'), 'col')
    replicated = P()

    def local_step(pair_tile, mask_tile, ln_in_scale, w_left, w_left_gate, w_right, w_right_gate, w_out_gate, ln_out_scale, w_out):
        _, cols, _ = pair_tile.shape
        half_cols = cols // 2
        row, z = lax.axis_index('row'), lax.axis_index('col')
        y, c = row // 2, row % 2
        half = z // 2
        w_a = jnp.concatenate([w_left, w_left_gate], axis=1).T
        w_b = jnp.concatenate([w_right, w_right_gate], axis=1).T
        gain_in, gain_out = ln_in_scale[None], ln_out_scale[None]

        inner = (z == 1) | (z == 2)
        inner_flag, outer_flag = inner.astype(jnp.int32)[None], (1 - inner.astype(jnp.int32))[None]

        def masked(pairs, mask, upper):
            pairs = jnp.where(upper, pairs[:, half_cols:], pairs[:, :half_cols])
            mask = jnp.where(upper, mask[:, half_cols:], mask[:, :half_cols])
            return jnp.where((mask != 0)[:, :, None], pairs, jnp.zeros((), BF16))

        t_b = masked(pair_tile, mask_tile, y == 0)
        t_a = masked(*after((pair_tile, mask_tile), t_b), y == 1)
        y_a = send(t_b, TO_Y)
        z_a = send(t_a, TO_Z)
        m_0 = send(t_a, ACROSS)
        x_gate = gate_in(pair_tile, gain_in)
        y_b = send(after(t_a, z_a), TO_Y)
        yz_a = send(after(y_a, x_gate), TO_Z)
        m_1 = send(y_a, ACROSS)
        z_b = send(after(t_b, yz_a), TO_Z)
        yz_b = send(after(z_a, y_b), TO_Y)

        keep = ((z % 2) == c).astype(jnp.int32)[None]
        seconds = (t_b, y_b), (z_b, yz_b)
        big = half_cols * 2 // 3
        small = half_cols - big
        x_own = norm((t_a, y_a), gain_in)
        a_1, x_1 = project(keep, (z_a, yz_a), None, gain_in, after(w_a, x_own), 0, big, with_x=True)
        a_2, x_2 = project(keep, (z_a, yz_a), None, gain_in, after(w_a, a_1), big, small, with_x=True)
        got_1, got_2 = send(a_1, ACROSS), send(a_2, ACROSS)
        give_0 = project_x(1 - keep, x_own, (x_1, x_2), after(w_b, a_2))
        a_0 = project(inner_flag, (m_0, m_1), (t_a, y_a), gain_in, after(w_a, give_0))
        a_pair = [(a_0, send(a_0, TO_CORE))]
        keep_0 = project_x(keep, x_own, (x_1, x_2), after(w_b, a_0))
        b_0 = [keep_0, send(give_0, TO_CORE)]
        done_0 = triangle(inner_flag, a_pair, b_0, gain_out)
        give_1 = project(1 - keep, *seconds, gain_in, after(w_b, done_0))
        keep_1 = project(keep, *seconds, gain_in, after(w_b, give_1))
        b_1 = [keep_1, send(give_1, TO_CORE)]
        b_parts = [b_0[0], b_1[0], b_0[1], b_1[1]]
        done_1 = triangle(inner_flag, a_pair, b_1, gain_out)
        pair_1 = [(got_1, send(after(got_1, keep_1), INNER_CORE)), (a_1, send(a_1, OUTER_CORE))]
        done_2 = triangle(inner_flag, pair_1, b_parts, after(gain_out, done_1))
        pair_2 = [(got_2, send(after(got_2, done_2), INNER_CORE)), (a_2, send(a_2, OUTER_CORE))]
        done_3 = triangle(inner_flag, pair_2, b_parts, after(gain_out, done_2))
        done = (done_0, done_1, done_2, done_3)

        got = [[send(v, home(from_y, n // 2)) for n, v in enumerate(done)] for from_y in (0, 1)]
        block_half = jnp.where(inner, 1 - half, half)
        turn = half ^ c
        own = (block_half == y) & (2 * half + c == z)
        pick = jnp.stack([turn + jnp.where(own & (y == from_y), 2, 0) for from_y in (0, 1)]).astype(jnp.int32)
        out = None
        for n, first, count in ((2, 0, big), (3, big, small)):
            candidates = [(tuple(got[s][:2]), (got[s][n],), (done_0, done_1), (done[n],)) for s in (0, 1)]
            out = finish(pick, pair_tile, x_gate, candidates, w_out, w_out_gate, first, count, out)
        return out

    return jax.shard_map(local_step, mesh=mesh, in_specs=(tile_spec, mask_spec) + (replicated,) * 8, out_specs=tile_spec, check_vma=False)
```
